256 devices in a mesh: grp: 8 (over z), sp: 32 (over y, x, core).
Axes of the slice: x: 4, y: 4, z: 8, core: 2. Of those that a mesh axis runs over, the one named last changes fastest.
Arguments:
- tokens: bfloat16 [16384, 2880], P(('grp', 'sp')), may hold values from -36 to 36
- query_weight: bfloat16 [2880, 2048], P(None, 'sp'), may hold values from -0.109375 to 0.109375
- key_value_weight: bfloat16 [2880, 1024], replicated, may hold values from -0.109375 to 0.109375
- block_places: int32 [32], replicated, may hold values from 0 to 31, each once
- sinks: float32 [32], replicated, may hold values from -1 to 5
Outputs:
- attended: bfloat16 [16384, 2048], P(('grp', 'sp'))
The draws below stay inside these ranges and needn't reach their ends.
Inputs may be any that keep to these rules, and one draw needn't show every extreme that they name: `block_places`: every sequence block appears once.
All inputs are finite; a program needn't handle non-finite values.
Results may differ from the reference program's by a relative error of at most 0.008.
The reference program's roundings to bfloat16 on the way count: a program that leaves them out, or rounds other values in their place, can miss the bound.
Values may be sent and summed in bfloat16 or wider, within the bound.
A program may use at most 128 MiB of HBM per device.

```python
import jax
import jax.numpy as jnp
from jax import lax

MODEL_WIDTH = 2880
QUERY_HEADS = 32
KEY_VALUE_HEADS = 8
HEAD_SIZE = 64
BLK = 512
NBLK = 32
SEQUENCE_TOKENS = 16384


def draw_tokens(key, part):
    base = jnp.clip(jax.random.normal(key, (SEQUENCE_TOKENS, MODEL_WIDTH), jnp.float32), -6.0, 6.0)
    return base.astype(jnp.bfloat16)


def block_levels(stream_key, extent, split, smallest, high):
    def one(position, shards_of):
        draws = jax.random.uniform(jax.random.fold_in(jax.random.fold_in(stream_key, 6), position), (shards_of,), jnp.float32, smallest / len(split), high / len(split))
        return jnp.repeat(jnp.exp(draws), extent[position] // shards_of).reshape((-1,) + (1,) * (len(extent) - position - 1))

    loudness = one(*split[0])
    for cut in split[1:]:
        loudness = loudness * one(*cut)
    return loudness


def scatter_about(stream_key, extent, width, most, cuts=(), kind=jnp.bfloat16):
    level = block_levels(stream_key, extent, cuts, -0.22, 0.18) if cuts else 1.0
    entries = jax.random.normal(stream_key, extent, jnp.float32) * width * level
    return jnp.minimum(jnp.maximum(entries, -most), most).astype(kind)


def setup_inputs(seed: int = 0) -> dict:
    keys = jax.random.split(jax.random.key(seed), 6)
    tokens = draw_tokens(jax.random.fold_in(keys[5], 71), 0)
    query_weight = scatter_about(keys[1], (MODEL_WIDTH, QUERY_HEADS * HEAD_SIZE), MODEL_WIDTH ** -0.5, 0.109375, ((1, 32),))
    key_value_weight = scatter_about(keys[2], (MODEL_WIDTH, 2 * KEY_VALUE_HEADS * HEAD_SIZE), MODEL_WIDTH ** -0.5, 0.109375)
    block_places = jax.random.permutation(keys[3], NBLK).astype(jnp.int32)
    sinks = jnp.clip(jax.random.uniform(keys[4], (QUERY_HEADS,), jnp.float32, -1.0, 5.0), -1.0, 5.0)
    return {"tokens": tokens, "query_weight": query_weight, "key_value_weight": key_value_weight, "block_places": block_places, "sinks": sinks}


rope_base = 150000.0
neg_large = -1.0e30


def rotate(vectors, angles):
    middle = vectors.shape[-1] // 2
    first_half = vectors[..., :middle]
    second_half = vectors[..., middle:]
    cosine = jnp.cos(angles)
    sine_part = jnp.sin(angles)
    return jnp.concatenate([first_half * cosine - second_half * sine_part, second_half * cosine + first_half * sine_part], axis=-1)


def reference(tokens, query_weight, key_value_weight, block_places, sinks):
    stored = jnp.arange(SEQUENCE_TOKENS, dtype=jnp.int32)
    blocks = stored // BLK
    places = block_places[blocks] * BLK + stored % BLK
    inverse = rope_base ** (-(jnp.arange(HEAD_SIZE // 2, dtype=jnp.float32) * 2.0) / HEAD_SIZE)
    angles = places.astype(jnp.float32)[:, None, None] * inverse[None, None, :]
    queries = jnp.dot(tokens, query_weight, preferred_element_type=jnp.float32).reshape(SEQUENCE_TOKENS, QUERY_HEADS, HEAD_SIZE)
    key_value_pair = jnp.dot(tokens, key_value_weight, preferred_element_type=jnp.float32)
    key_head_rows = key_value_pair[:, :KEY_VALUE_HEADS * HEAD_SIZE].reshape(SEQUENCE_TOKENS, KEY_VALUE_HEADS, HEAD_SIZE)
    value_head_rows = key_value_pair[:, KEY_VALUE_HEADS * HEAD_SIZE:].reshape(SEQUENCE_TOKENS, KEY_VALUE_HEADS, HEAD_SIZE).astype(jnp.bfloat16)
    queries = rotate(queries, angles).astype(jnp.bfloat16)
    key_head_rows = rotate(key_head_rows, angles).astype(jnp.bfloat16)
    query_sharing = QUERY_HEADS // KEY_VALUE_HEADS
    score_scale = HEAD_SIZE ** -0.5

    def single_head(head_number):
        head_keys = lax.dynamic_index_in_dim(key_head_rows, head_number, 1, keepdims=False).astype(jnp.float32)
        head_values = lax.dynamic_index_in_dim(value_head_rows, head_number, 1, keepdims=False).astype(jnp.float32)
        head_queries = lax.dynamic_slice_in_dim(queries, head_number * query_sharing, query_sharing, 1)
        head_sinks = lax.dynamic_slice_in_dim(sinks, head_number * query_sharing, query_sharing, 0)

        def one_block(query_block):
            first_row = query_block * BLK
            query_rows = lax.dynamic_slice_in_dim(head_queries, first_row, BLK, 0).astype(jnp.float32)
            row_places = lax.dynamic_slice_in_dim(places, first_row, BLK, 0)
            scores = jnp.einsum("qgd,kd->gqk", query_rows, head_keys) * score_scale
            allowed = places[None, :] <= row_places[:, None]
            scores = jnp.where(allowed[None], scores, neg_large)
            highest = jnp.maximum(jnp.max(scores, axis=-1, keepdims=True), head_sinks[:, None, None])
            weights = jnp.where(allowed[None], jnp.exp(scores - highest), 0.0)
            totals = jnp.sum(weights, axis=-1) + jnp.exp(head_sinks[:, None] - highest[..., 0])
            rounded = lax.optimization_barrier(weights.astype(jnp.bfloat16)).astype(jnp.float32)
            mixture = jnp.einsum("gqk,kd->qgd", rounded, head_values)
            return mixture / jnp.transpose(totals)[:, :, None]

        return lax.map(one_block, jnp.arange(SEQUENCE_TOKENS // BLK, dtype=jnp.int32))

    layer_output = lax.map(single_head, jnp.arange(KEY_VALUE_HEADS, dtype=jnp.int32))
    layer_output = jnp.transpose(layer_output, (1, 2, 0, 3, 4)).reshape(SEQUENCE_TOKENS, QUERY_HEADS * HEAD_SIZE)
    return layer_output.astype(jnp.bfloat16)
```

```python
import math

import jax
import jax.numpy as jnp
import numpy as np
from jax import lax
from jax.experimental import pallas as pl
from jax.experimental.pallas import tpu as pltpu
from jax.sharding import PartitionSpec as P

MESH = pl.DeviceIdType.MESH
BF16, F32, I32 = jnp.bfloat16, jnp.float32, jnp.int32
WIDTH = 2880
HEAD = 64
BLK = 512
NBLK = 32
SCALE_LOG2 = HEAD**-0.5 * math.log2(math.e)
NEG = -1e30
VMEM = pl.BlockSpec(memory_space=pltpu.VMEM)
HBM = pl.BlockSpec(memory_space=pltpu.HBM)
SMEM = pl.BlockSpec(memory_space=pltpu.SMEM)
INVERSE = (150000.0 ** (-(np.arange(32, dtype=np.float64) * 2.0) / HEAD)).astype(np.float32)


def place():
    z = lax.axis_index("grp")
    s = lax.axis_index("sp")
    return z, s // 8, (s // 2) % 4, s % 2


def dev(z, y, x, c):
    return (z, (y * 4 + x) * 2 + c)


def dot(a, b, ca, cb):
    return lax.dot_general(a, b, (((ca,), (cb,)), ((), ())), preferred_element_type=F32)


def barrier_with(peers):
    sem = pltpu.get_barrier_semaphore()
    for peer in peers:
        pl.semaphore_signal(sem, inc=1, device_id=peer, device_id_type=MESH)
    pl.semaphore_wait(sem, len(peers))


def kv_kernel(places, inv_ref, tok_ref, wk_ref, wv_ref, wq_ref, kvp_ref, wqt_ref, cos_s, sin_s):
    z, y, x, c = place()
    lane = lax.broadcasted_iota(I32, (64, 128), 1)

    @pl.when(pl.program_id(0) == 0)
    def _():
        base = places[z * 4 + y] * BLK + (x * 2 + c) * 64
        pos = (base + lax.broadcasted_iota(I32, (64, 128), 0)).astype(F32)
        angle = pos * inv_ref[...]
        cos_s[...] = jnp.cos(angle)
        sin_s[...] = jnp.where(lane % 64 < 32, -1.0, 1.0) * jnp.sin(angle)
        eye = (
            lax.broadcasted_iota(I32, (64, 64), 0) == lax.broadcasted_iota(I32, (64, 64), 1)
        ).astype(BF16)
        wqt_ref[...] = dot(eye, wq_ref[...], 1, 1).astype(BF16)

    k = jnp.dot(tok_ref[...], wk_ref[...], preferred_element_type=F32)
    v = jnp.dot(tok_ref[...], wv_ref[...], preferred_element_type=F32)
    swapped = jnp.where(lane % 64 < 32, pltpu.roll(k, 96, 1), pltpu.roll(k, 32, 1))
    k = k * cos_s[...] + swapped * sin_s[...]
    kvp_ref[0] = jnp.where(lane < 64, k, pltpu.roll(v, 64, 1)).astype(BF16)
    kvp_ref[1] = jnp.where(lane < 64, pltpu.roll(k, 64, 1), v).astype(BF16)


def kv_project(places, tokens, kvw, wq):
    inv = jnp.asarray(np.tile(INVERSE, 4)[None, :])
    return pl.pallas_call(
        kv_kernel,
        grid=(4,),
        in_specs=[
            SMEM,
            pl.BlockSpec((1, 128), lambda n: (0, 0)),
            pl.BlockSpec((64, WIDTH), lambda n: (0, 0)),
            pl.BlockSpec((WIDTH, 128), lambda n: (0, n)),
            pl.BlockSpec((WIDTH, 128), lambda n: (0, 4 + n)),
            pl.BlockSpec((WIDTH, 64), lambda n: (0, 0)),
        ],
        out_specs=[
            pl.BlockSpec((2, 64, 128), lambda n: (n, 0, 0)),
            pl.BlockSpec((64, WIDTH), lambda n: (0, 0)),
        ],
        out_shape=[
            jax.ShapeDtypeStruct((8, 64, 128), BF16),
            jax.ShapeDtypeStruct((64, WIDTH), BF16),
        ],
        scratch_shapes=[pltpu.VMEM((64, 128), F32), pltpu.VMEM((64, 128), F32)],
        name="kv_project",
    )(places, inv, tokens, kvw, kvw, wq)


class Ring:
    def __init__(self, at, me, right, left, send, recv, first):
        self.at, self.me, self.right, self.left = at, me, right, left
        self.send, self.recv, self.first = send, recv, first
        self.prev, self.next, self.opp = (me + 3) % 4, (me + 1) % 4, (me + 2) % 4

    def copy(self, piece, half, target, k):
        ref = self.at(piece, half)
        return pltpu.make_async_remote_copy(
            src_ref=ref,
            dst_ref=ref,
            send_sem=self.send.at[self.first + k],
            recv_sem=self.recv.at[self.first + k],
            device_id=target,
            device_id_type=MESH,
        )

    def start(self):
        self.copy(self.me, 0, self.right, 0).start()
        self.copy(self.me, 1, self.left, 2).start()
        self.copy(self.me, 1, self.right, 1).start()
        self.copy(self.me, 0, self.left, 3).start()

    def forward(self):
        self.copy(self.prev, 0, self.right, 0).wait_recv()
        self.copy(self.prev, 0, self.right, 4).start()
        self.copy(self.next, 1, self.left, 2).wait_recv()
        self.copy(self.next, 1, self.left, 5).start()

    def near(self):
        self.copy(self.prev, 1, self.right, 1).wait_recv()
        self.copy(self.next, 0, self.left, 3).wait_recv()

    def far(self):
        self.copy(self.opp, 0, self.right, 4).wait_recv()
        self.copy(self.opp, 1, self.left, 5).wait_recv()

    def drain(self):
        self.copy(self.me, 0, self.right, 0).wait_send()
        self.copy(self.me, 1, self.right, 1).wait_send()
        self.copy(self.me, 1, self.left, 2).wait_send()
        self.copy(self.me, 0, self.left, 3).wait_send()
        self.copy(self.prev, 0, self.right, 4).wait_send()
        self.copy(self.next, 1, self.left, 5).wait_send()


def gather_kernel(tok_hbm, wqt_hbm, kvp_hbm, tok, wts, kv, kvp, lsem, send, recv, zsend, zrecv, psend, precv):
    z, y, x, c = place()
    o = 1 - c
    a, b = x * o + y * c, y * o + x * c
    partner = dev(z, y, x, o)
    ring_y = (dev(z, (y + 1) % 4, x, c), dev(z, (y + 3) % 4, x, c))
    ring_x = (dev(z, y, (x + 1) % 4, c), dev(z, y, (x + 3) % 4, c))
    others = [dev((z + d) % 8, y, x, c) for d in range(1, 8)]

    own = [
        pltpu.make_async_copy(tok_hbm, tok.at[y], lsem.at[0]),
        pltpu.make_async_copy(wqt_hbm, wts.at[x, c], lsem.at[1]),
        pltpu.make_async_copy(kvp_hbm, kvp, lsem.at[2]),
        pltpu.make_async_copy(kvp_hbm.at[z], kv.at[c, b, a, z], lsem.at[3]),
    ]
    for copy in own:
        copy.start()
    barrier_with([*ring_y, *ring_x, partner, *others])

    tok_ring = Ring(lambda p, h: tok.at[p, h], y, *ring_y, send, recv, 0)
    wts_ring = Ring(lambda p, h: wts.at[p, c, h], x, *ring_x, send, recv, 6)
    near = [
        dev(z, (y + c) % 4, (x + o) % 4, c),
        dev(z, (y + 3 * c) % 4, (x + 3 * o) % 4, c),
    ]
    wide = [
        dev(z, (y + o) % 4, (x + c) % 4, c),
        dev(z, (y + 3 * o) % 4, (x + 3 * c) % 4, c),
    ]
    kv1_ring = Ring(lambda p, h: kv.at[c, b, p, pl.ds(4 * h, 4)], a, *near, send, recv, 12)
    kv2_ring = Ring(lambda p, h: kv.at[c, p, :, pl.ds(4 * h, 4)], b, *wide, send, recv, 18)

    def to_partner(ref, k):
        return pltpu.make_async_remote_copy(
            src_ref=ref,
            dst_ref=ref,
            send_sem=psend.at[k],
            recv_sem=precv.at[k],
            device_id=partner,
            device_id_type=MESH,
        )

    own[0].wait()
    tok_ring.start()
    own[1].wait()
    wts_ring.start()
    to_partner(wts.at[x, c], 0).start()
    own[2].wait()
    own[3].wait()
    zs = []
    for d in range(1, 8):
        zz = (z + d) % 8
        copy = pltpu.make_async_remote_copy(
            src_ref=kvp.at[zz],
            dst_ref=kv.at[c, b, a, z],
            send_sem=zsend.at[d - 1],
            recv_sem=zrecv.at[d - 1],
            device_id=others[d - 1],
            device_id_type=MESH,
        )
        copy.start()
        zs.append(copy)
    for d in range(1, 8):
        zz = (z + 8 - d) % 8
        pltpu.make_async_remote_copy(
            src_ref=kvp.at[zz],
            dst_ref=kv.at[c, b, a, zz],
            send_sem=zsend.at[d - 1],
            recv_sem=zrecv.at[d - 1],
            device_id=others[d - 1],
            device_id_type=MESH,
        ).wait_recv()
    kv1_ring.start()

    wts_ring.forward()
    tok_ring.forward()
    wts_ring.near()
    to_partner(wts.at[(x + 3) % 4, c], 1).start()
    to_partner(wts.at[(x + 1) % 4, c], 2).start()
    tok_ring.near()
    kv1_ring.forward()
    kv1_ring.near()
    kv1_ring.far()
    kv2_ring.start()
    to_partner(kv.at[c, b], 4).start()
    wts_ring.far()
    to_partner(wts.at[(x + 2) % 4, c], 3).start()
    tok_ring.far()
    kv2_ring.forward()
    kv2_ring.near()
    to_partner(kv.at[c, (b + 3) % 4], 5).start()
    to_partner(kv.at[c, (b + 1) % 4], 6).start()
    kv2_ring.far()
    to_partner(kv.at[c, (b + 2) % 4], 7).start()

    def from_partner(ref, k):
        pltpu.make_async_remote_copy(
            src_ref=ref,
            dst_ref=ref,
            send_sem=psend.at[k],
            recv_sem=precv.at[k],
            device_id=partner,
            device_id_type=MESH,
        ).wait_recv()

    from_partner(wts.at[x, o], 0)
    from_partner(wts.at[(x + 3) % 4, o], 1)
    from_partner(wts.at[(x + 1) % 4, o], 2)
    from_partner(wts.at[(x + 2) % 4, o], 3)
    from_partner(kv.at[o, a], 4)
    from_partner(kv.at[o, (a + 3) % 4], 5)
    from_partner(kv.at[o, (a + 1) % 4], 6)
    from_partner(kv.at[o, (a + 2) % 4], 7)
    for ring in (tok_ring, wts_ring, kv1_ring, kv2_ring):
        ring.drain()
    for copy in zs:
        copy.wait_send()
    to_partner(wts.at[x, c], 0).wait_send()
    to_partner(wts.at[(x + 3) % 4, c], 1).wait_send()
    to_partner(wts.at[(x + 1) % 4, c], 2).wait_send()
    to_partner(wts.at[(x + 2) % 4, c], 3).wait_send()
    to_partner(kv.at[c, b], 4).wait_send()
    to_partner(kv.at[c, (b + 3) % 4], 5).wait_send()
    to_partner(kv.at[c, (b + 1) % 4], 6).wait_send()
    to_partner(kv.at[c, (b + 2) % 4], 7).wait_send()


def gather(tokens, wqt, kvp):
    return pl.pallas_call(
        gather_kernel,
        in_specs=[HBM, HBM, HBM],
        out_specs=[VMEM, VMEM, VMEM],
        out_shape=[
            jax.ShapeDtypeStruct((4, 2, 32, WIDTH), BF16),
            jax.ShapeDtypeStruct((4, 2, 2, 32, WIDTH), BF16),
            jax.ShapeDtypeStruct((2, 4, 4, 8, 64, 128), BF16),
        ],
        scratch_shapes=[
            pltpu.VMEM((8, 64, 128), BF16),
            pltpu.SemaphoreType.DMA((4,)),
            pltpu.SemaphoreType.DMA((24,)),
            pltpu.SemaphoreType.DMA((24,)),
            pltpu.SemaphoreType.DMA((7,)),
            pltpu.SemaphoreType.DMA((7,)),
            pltpu.SemaphoreType.DMA((8,)),
            pltpu.SemaphoreType.DMA((8,)),
        ],
        compiler_params=pltpu.CompilerParams(collective_id=1, has_side_effects=True),
        name="gather",
    )(tokens.reshape(2, 32, WIDTH), wqt.reshape(2, 32, WIDTH), kvp)


def query_kernel(places, inv_ref, tok, wts, out, stage, send, recv):
    z, y, x, c = place()
    peers = [
        dev((z + dz) % 8, (y + dy) % 4, x, c)
        for dz in range(8)
        for dy in range(4)
        if dz or dy
    ]
    sem = pltpu.get_barrier_semaphore()
    for peer in peers:
        pl.semaphore_signal(sem, inc=1, device_id=peer, device_id_type=MESH)

    lane = lax.broadcasted_iota(I32, (32, 256), 1)
    row_block = jnp.where(
        lane < 128,
        jnp.where(lane < 64, places[z * 4], places[z * 4 + 1]),
        jnp.where(lane < 192, places[z * 4 + 2], places[z * 4 + 3]),
    )
    pos = row_block * BLK + (x * 2 + c) * 64 + lane % 64
    angle = pos.astype(F32) * jnp.concatenate([inv_ref[...], inv_ref[...]], axis=1)
    cosine, sine = jnp.cos(angle), jnp.sin(angle)
    t = tok[...].reshape(256, WIDTH)

    def target(k):
        return 2 * y + k // 4, k % 4

    def message(k):
        zz, yy = target(k)
        return pltpu.make_async_remote_copy(
            src_ref=stage.at[k],
            dst_ref=out.at[z],
            send_sem=send.at[k],
            recv_sem=recv.at[z],
            device_id=dev(zz, yy, x, c),
            device_id_type=MESH,
        )

    def away(k):
        zz, yy = target(k)
        return jnp.logical_or(zz != z, yy != y)

    for half in range(2):
        w = wts[2 * half : 2 * half + 2].reshape(256, WIDTH)
        q = dot(w, t, 1, 1)
        for i in range(4):
            k = half * 4 + i
            lo, hi = q[i * 64 : i * 64 + 32], q[i * 64 + 32 : i * 64 + 64]
            stage[k, :32] = (lo * cosine - hi * sine).astype(BF16)
            stage[k, 32:] = (hi * cosine + lo * sine).astype(BF16)
        if half == 0:
            pl.semaphore_wait(sem, len(peers))
        for i in range(4):
            k = half * 4 + i

            @pl.when(away(k))
            def _():
                message(k).start()

            @pl.when(jnp.logical_not(away(k)))
            def _():
                out[z] = stage[k]

    for g in range(8):

        @pl.when(jnp.logical_or(g != z, z // 2 != y))
        def _():
            pltpu.make_async_remote_copy(
                src_ref=stage.at[0],
                dst_ref=out.at[g],
                send_sem=send.at[0],
                recv_sem=recv.at[g],
                device_id=dev(g, z // 2, x, c),
                device_id_type=MESH,
            ).wait_recv()

    for k in range(8):

        @pl.when(away(k))
        def _():
            message(k).wait_send()


def query_project(places, tok, wts):
    inv = jnp.asarray(np.tile(INVERSE[:, None], (1, 128)))
    return pl.pallas_call(
        query_kernel,
        in_specs=[SMEM, VMEM, VMEM, VMEM],
        out_specs=VMEM,
        out_shape=jax.ShapeDtypeStruct((8, 64, 256), BF16),
        scratch_shapes=[
            pltpu.VMEM((8, 64, 256), BF16),
            pltpu.SemaphoreType.DMA((8,)),
            pltpu.SemaphoreType.DMA((8,)),
        ],
        compiler_params=pltpu.CompilerParams(collective_id=2, has_side_effects=True),
        name="query_project",
    )(places, inv, tok, wts)


def attend_kernel(places, sinks, q_ref, kv_ref, o_ref, order, vt, qt, gap, s0, s1):
    z, y, x, c = place()
    offset = (x * 2 + c) * 64
    for b in range(NBLK):
        order[places[b]] = b
    sink = sinks[z * 4 + y] * math.log2(math.e)

    key = lax.broadcasted_iota(I32, (BLK, 256), 0)
    col = lax.broadcasted_iota(I32, (BLK, 256), 1)
    key = ((key >> 6) & 3) * 128 + (key >> 8) * 64 + (key & 63)
    gap[...] = key - ((col >> 6) * BLK + offset + (col & 63))

    def keys_of(i):
        b = order[i]
        g, r = b // 4, b % 4
        k0 = kv_ref[0, r, :, g].reshape(256, 128)
        k1 = kv_ref[1, :, r, g].reshape(256, 128)
        return jnp.concatenate([k0, k1], axis=0)

    row = lax.broadcasted_iota(I32, (80, 128), 0)
    pick = jnp.logical_and(row < 64, lax.broadcasted_iota(I32, (80, 128), 1) == row + 64)
    pick = jnp.where(pick, 1.0, 0.0).astype(BF16)
    wide_row = lax.broadcasted_iota(I32, (80, BLK), 0)

    def values_of(i, _):
        vt[i] = jnp.where(wide_row < 64, dot(pick, keys_of(i), 1, 1), 1.0).astype(BF16)
        return 0

    lax.fori_loop(0, NBLK, values_of, 0)
    lane = lax.broadcasted_iota(I32, (64, 256), 1)

    def tile(j, _):
        q = jnp.zeros((64, 256), F32)
        for a in range(4):
            b = order[4 * j + a]
            part = pltpu.roll(q_ref[b // 4].astype(F32), ((a + 4 - b % 4) % 4) * 64, 1)
            q = jnp.where(lane >> 6 == a, part, q)
        qt[:64] = q.astype(BF16)
        qt[64:] = jnp.zeros((64, 256), BF16)

        def produce(i, s, masked):
            scores = dot(keys_of(i), qt[...], 1, 0) * SCALE_LOG2
            if masked:
                scores = jnp.where(gap[...] <= (4 * j - i) * BLK, scores, NEG)
            s[...] = scores
            return jnp.max(scores, axis=0, keepdims=True)

        def consume(i, s, peak, m, acc):
            new = jnp.maximum(m, peak)
            w = jnp.exp2(s[...] - new).astype(BF16)
            return new, acc * jnp.exp2(m - new) + dot(vt[i], w, 1, 0)

        def pair(masked):
            def step(t, carry):
                m, acc, peak0 = carry
                peak1 = produce(2 * t + 1, s1, masked)
                m, acc = consume(2 * t, s0, peak0, m, acc)
                peak0 = produce(2 * t + 2, s0, masked)
                m, acc = consume(2 * t + 1, s1, peak1, m, acc)
                return m, acc, peak0

            return step

        m = jnp.full((1, 256), sink, F32)
        acc = jnp.where(lax.broadcasted_iota(I32, (80, 256), 0) < 64, 0.0, 1.0)
        peak = produce(0, s0, True)
        free = jnp.maximum(2 * j - 1, 0)
        carry = lax.fori_loop(0, free, pair(False), (m, acc, peak))
        m, acc, peak0 = lax.fori_loop(free, 2 * j + 1, pair(True), carry)
        peak1 = produce(4 * j + 3, s1, True)
        m, acc = consume(4 * j + 2, s0, peak0, m, acc)
        m, acc = consume(4 * j + 3, s1, peak1, m, acc)

        out = acc[:64] / acc[64:65]
        out = jnp.concatenate([out, jnp.zeros((64, 256), F32)], axis=0).T
        for a in range(4):
            top, low = out[64 * a : 64 * a + 32], out[64 * a + 32 : 64 * a + 64]
            o_ref[order[4 * j + a]] = (top + pltpu.roll(low, 64, 1)).astype(BF16)
        return 0

    lax.fori_loop(0, NBLK // 4, tile, 0)


def attend(places, sinks, q, kv):
    return pl.pallas_call(
        attend_kernel,
        in_specs=[SMEM, SMEM, VMEM, VMEM],
        out_specs=VMEM,
        out_shape=jax.ShapeDtypeStruct((NBLK, 32, 128), BF16),
        scratch_shapes=[
            pltpu.SMEM((NBLK,), I32),
            pltpu.VMEM((NBLK, 80, BLK), BF16),
            pltpu.VMEM((128, 256), BF16),
            pltpu.VMEM((BLK, 256), I32),
            pltpu.VMEM((BLK, 256), F32),
            pltpu.VMEM((BLK, 256), F32),
        ],
        name="attend",
    )(places, sinks, q, kv)


def return_kernel(o_hbm, out, held, own, lsem, send, recv):
    z, y, x, c = place()
    offsets = [(dz, dy) for dz in range(8) for dy in range(4) if dz or dy]
    local = [
        pltpu.make_async_copy(o_hbm, own, lsem.at[0]),
        pltpu.make_async_copy(o_hbm.at[z * 4 + y], held.at[z * 4 + y], lsem.at[1]),
    ]
    for copy in local:
        copy.start()
    barrier_with([dev((z + dz) % 8, (y + dy) % 4, x, c) for dz, dy in offsets])
    for copy in local:
        copy.wait()
    copies = []
    for k, (dz, dy) in enumerate(offsets):
        zz, yy = (z + dz) % 8, (y + dy) % 4
        copy = pltpu.make_async_remote_copy(
            src_ref=own.at[zz * 4 + yy],
            dst_ref=held.at[z * 4 + y],
            send_sem=send.at[k],
            recv_sem=recv.at[k],
            device_id=dev(zz, yy, x, c),
            device_id_type=MESH,
        )
        copy.start()
        copies.append(copy)
    for k, (dz, dy) in enumerate(offsets):
        zz, yy = (z + 8 - dz) % 8, (y + 4 - dy) % 4
        pltpu.make_async_remote_copy(
            src_ref=own.at[0],
            dst_ref=held.at[zz * 4 + yy],
            send_sem=send.at[k],
            recv_sem=recv.at[k],
            device_id=dev(zz, yy, x, c),
            device_id_type=MESH,
        ).wait_recv()
    lane = lax.broadcasted_iota(I32, (32, 128), 1)
    for k in range(16):
        p, q = held[2 * k].astype(F32), held[2 * k + 1].astype(F32)
        cols = pl.ds(128 * k, 128)
        out[:32, cols] = jnp.where(lane < 64, p, pltpu.roll(q, 64, 1)).astype(BF16)
        out[32:, cols] = jnp.where(lane < 64, pltpu.roll(p, 64, 1), q).astype(BF16)
    for copy in copies:
        copy.wait_send()


def send_back(o):
    return pl.pallas_call(
        return_kernel,
        in_specs=[HBM],
        out_specs=VMEM,
        out_shape=jax.ShapeDtypeStruct((64, 2048), BF16),
        scratch_shapes=[
            pltpu.VMEM((NBLK, 32, 128), BF16),
            pltpu.VMEM((NBLK, 32, 128), BF16),
            pltpu.SemaphoreType.DMA((2,)),
            pltpu.SemaphoreType.DMA((31,)),
            pltpu.SemaphoreType.DMA((31,)),
        ],
        compiler_params=pltpu.CompilerParams(collective_id=3, has_side_effects=True),
        name="send_back",
    )(o)


def per_device(tokens, query_weight, key_value_weight, block_places, sinks):
    kvp, wqt = kv_project(block_places, tokens, key_value_weight, query_weight)
    tok, wts, kv = gather(tokens, wqt, kvp)
    q = query_project(block_places, tok, wts)
    o = attend(block_places, sinks, q, kv)
    return send_back(o)


def solution(mesh):
    in_specs = (P(("grp", "sp"), None), P(None, "sp"), P(), P(), P())
    return jax.shard_map(
        per_device,
        mesh=mesh,
        in_specs=in_specs,
        out_specs=P(("grp", "sp"), None),
        check_vma=False,
    )
```

```python
import math

import jax
import jax.numpy as jnp
import numpy as np
from jax import lax
from jax.experimental import pallas as pl
from jax.experimental.pallas import tpu as pltpu
from jax.sharding import PartitionSpec as P

MESH = pl.DeviceIdType.MESH
BF16, F32, I32 = jnp.bfloat16, jnp.float32, jnp.int32
WIDTH = 2880
HEAD = 64
BLK = 512
NBLK = 32
SCALE_LOG2 = HEAD**-0.5 * math.log2(math.e)
NEG = -1e30
VMEM = pl.BlockSpec(memory_space=pltpu.VMEM)
HBM = pl.BlockSpec(memory_space=pltpu.HBM)
SMEM = pl.BlockSpec(memory_space=pltpu.SMEM)
OFFSETS = [(dz, dy) for dz in range(8) for dy in range(4) if dz or dy]
INVERSE = (150000.0 ** (-(np.arange(32, dtype=np.float64) * 2.0) / HEAD)).astype(np.float32)


def place():
    z = lax.axis_index("grp")
    s = lax.axis_index("sp")
    return z, s // 8, (s // 2) % 4, s % 2


def dev(z, y, x, c):
    return (z, (y * 4 + x) * 2 + c)


def dot(a, b, ca, cb):
    return lax.dot_general(a, b, (((ca,), (cb,)), ((), ())), preferred_element_type=F32)


def barrier_with(peers):
    sem = pltpu.get_barrier_semaphore()
    for peer in peers:
        pl.semaphore_signal(sem, inc=1, device_id=peer, device_id_type=MESH)
    pl.semaphore_wait(sem, len(peers))


class Ring:
    def __init__(self, at, me, right, left, send, recv, first):
        self.at, self.me, self.right, self.left = at, me, right, left
        self.send, self.recv, self.first = send, recv, first
        self.prev, self.next, self.opp = (me + 3) % 4, (me + 1) % 4, (me + 2) % 4

    def copy(self, piece, half, target, k):
        ref = self.at(piece, half)
        return pltpu.make_async_remote_copy(
            src_ref=ref,
            dst_ref=ref,
            send_sem=self.send.at[self.first + k],
            recv_sem=self.recv.at[self.first + k],
            device_id=target,
            device_id_type=MESH,
        )

    def start(self):
        self.copy(self.me, 0, self.right, 0).start()
        self.copy(self.me, 1, self.left, 2).start()
        self.copy(self.me, 1, self.right, 1).start()
        self.copy(self.me, 0, self.left, 3).start()

    def forward(self):
        self.copy(self.prev, 0, self.right, 0).wait_recv()
        self.copy(self.prev, 0, self.right, 4).start()
        self.copy(self.next, 1, self.left, 2).wait_recv()
        self.copy(self.next, 1, self.left, 5).start()

    def near(self):
        self.copy(self.prev, 1, self.right, 1).wait_recv()
        self.copy(self.next, 0, self.left, 3).wait_recv()

    def far(self):
        self.copy(self.opp, 0, self.right, 4).wait_recv()
        self.copy(self.opp, 1, self.left, 5).wait_recv()

    def drain(self):
        self.copy(self.me, 0, self.right, 0).wait_send()
        self.copy(self.me, 1, self.right, 1).wait_send()
        self.copy(self.me, 1, self.left, 2).wait_send()
        self.copy(self.me, 0, self.left, 3).wait_send()
        self.copy(self.prev, 0, self.right, 4).wait_send()
        self.copy(self.next, 1, self.left, 5).wait_send()


def prepare_kernel(
    places, inv_row, inv_col, tok_hbm, wqt_hbm, kvw_hbm, q_out, kv,
    tok, wts, kvw, kvp, stage, angles, lsem, send, recv, zsend, zrecv, psend, precv, qsend, qrecv,
):
    z, y, x, c = place()
    o = 1 - c
    a, b = x * o + y * c, y * o + x * c
    partner = dev(z, y, x, o)
    ring_y = (dev(z, (y + 1) % 4, x, c), dev(z, (y + 3) % 4, x, c))
    ring_x = (dev(z, y, (x + 1) % 4, c), dev(z, y, (x + 3) % 4, c))
    others = [dev((z + d) % 8, y, x, c) for d in range(1, 8)]
    peers = [dev((z + dz) % 8, (y + dy) % 4, x, c) for dz, dy in OFFSETS]
    peers += [*ring_x, partner]

    ready = pltpu.get_barrier_semaphore()
    for peer in peers:
        pl.semaphore_signal(ready, inc=1, device_id=peer, device_id_type=MESH)

    own = [
        pltpu.make_async_copy(tok_hbm, tok.at[y], lsem.at[0]),
        pltpu.make_async_copy(wqt_hbm, wts.at[x, c], lsem.at[1]),
    ]
    for n in range(4):
        cols = pl.ds(256 * n, 256)
        own.append(pltpu.make_async_copy(kvw_hbm.at[:, cols], kvw.at[:, cols], lsem.at[2 + n]))
    for n in (0, 1, 2, 4, 3, 5):
        own[n].start()

    lane = lax.broadcasted_iota(I32, (64, 128), 1)
    base = places[z * 4 + y] * BLK + (x * 2 + c) * 64
    angle = (base + lax.broadcasted_iota(I32, (64, 128), 0)).astype(F32) * inv_row[...]
    cosine = jnp.cos(angle)
    sine = jnp.where(lane % 64 < 32, -1.0, 1.0) * jnp.sin(angle)
    own[0].wait()
    rows = tok[y].reshape(64, WIDTH)
    for n in range(2):
        own[2 + n].wait()
        own[4 + n].wait()
        keys = jnp.dot(rows, kvw[:, 256 * n : 256 * n + 256], preferred_element_type=F32)
        values = jnp.dot(rows, kvw[:, 512 + 256 * n : 768 + 256 * n], preferred_element_type=F32)
        for p in range(2):
            k, v = keys[:, 128 * p : 128 * p + 128], values[:, 128 * p : 128 * p + 128]
            swapped = jnp.where(lane % 64 < 32, pltpu.roll(k, 96, 1), pltpu.roll(k, 32, 1))
            k = k * cosine + swapped * sine
            kvp[4 * n + 2 * p] = jnp.where(lane < 64, k, pltpu.roll(v, 64, 1)).astype(BF16)
            kvp[4 * n + 2 * p + 1] = jnp.where(lane < 64, pltpu.roll(k, 64, 1), v).astype(BF16)
    kv[c, b, a, z] = kvp[z]

    col = lax.broadcasted_iota(I32, (32, 256), 1)
    block = jnp.where(
        col < 128,
        jnp.where(col < 64, places[z * 4], places[z * 4 + 1]),
        jnp.where(col < 192, places[z * 4 + 2], places[z * 4 + 3]),
    )
    angle = (block * BLK + (x * 2 + c) * 64 + col % 64).astype(F32)
    angle = angle * jnp.concatenate([inv_col[...], inv_col[...]], axis=1)
    angles[0], angles[1] = jnp.cos(angle), jnp.sin(angle)
    own[1].wait()
    pl.semaphore_wait(ready, len(peers))

    tok_ring = Ring(lambda p, h: tok.at[p, h], y, *ring_y, send, recv, 0)
    wts_ring = Ring(lambda p, h: wts.at[p, c, h], x, *ring_x, send, recv, 6)
    near = [
        dev(z, (y + c) % 4, (x + o) % 4, c),
        dev(z, (y + 3 * c) % 4, (x + 3 * o) % 4, c),
    ]
    wide = [
        dev(z, (y + o) % 4, (x + c) % 4, c),
        dev(z, (y + 3 * o) % 4, (x + 3 * c) % 4, c),
    ]
    kv1_ring = Ring(lambda p, h: kv.at[c, b, p, pl.ds(4 * h, 4)], a, *near, send, recv, 12)
    kv2_ring = Ring(lambda p, h: kv.at[c, p, :, pl.ds(4 * h, 4)], b, *wide, send, recv, 18)

    def with_partner(ref, k):
        return pltpu.make_async_remote_copy(
            src_ref=ref,
            dst_ref=ref,
            send_sem=psend.at[k],
            recv_sem=precv.at[k],
            device_id=partner,
            device_id_type=MESH,
        )

    def exchange(d, head, source):
        return pltpu.make_async_remote_copy(
            src_ref=kvp.at[head],
            dst_ref=kv.at[c, b, a, source],
            send_sem=zsend.at[d - 1],
            recv_sem=zrecv.at[d - 1],
            device_id=others[d - 1],
            device_id_type=MESH,
        )

    tok_ring.start()
    wts_ring.start()
    for d in range(1, 8):
        exchange(d, (z + d) % 8, z).start()
    with_partner(wts.at[x, c], 0).start()
    for d in range(1, 8):
        exchange(d, z, (z + 8 - d) % 8).wait_recv()
    kv1_ring.start()

    wts_ring.forward()
    tok_ring.forward()
    wts_ring.near()
    with_partner(wts.at[(x + 3) % 4, c], 1).start()
    with_partner(wts.at[(x + 1) % 4, c], 2).start()
    tok_ring.near()
    kv1_ring.forward()
    wts_ring.far()
    with_partner(wts.at[(x + 2) % 4, c], 3).start()
    kv1_ring.near()
    kv1_ring.far()
    kv2_ring.start()
    with_partner(kv.at[c, b], 4).start()
    tok_ring.far()
    with_partner(wts.at[x, o], 0).wait_recv()
    with_partner(wts.at[(x + 3) % 4, o], 1).wait_recv()
    with_partner(wts.at[(x + 1) % 4, o], 2).wait_recv()
    with_partner(wts.at[(x + 2) % 4, o], 3).wait_recv()

    def message(k):
        return pltpu.make_async_remote_copy(
            src_ref=stage.at[k],
            dst_ref=q_out.at[z],
            send_sem=qsend.at[k],
            recv_sem=qrecv.at[z],
            device_id=dev(2 * y + k // 4, k % 4, x, c),
            device_id_type=MESH,
        )

    def away(k):
        return jnp.logical_or(2 * y + k // 4 != z, k % 4 != y)

    rows = tok[...].reshape(256, WIDTH)
    for half in range(2):
        w = wts[2 * half : 2 * half + 2].reshape(256, WIDTH)
        q = dot(w, rows, 1, 1)
        for i in range(4):
            k = half * 4 + i
            lo, hi = q[i * 64 : i * 64 + 32], q[i * 64 + 32 : i * 64 + 64]
            stage[k, :32] = (lo * angles[0] - hi * angles[1]).astype(BF16)
            stage[k, 32:] = (hi * angles[0] + lo * angles[1]).astype(BF16)
    for k in range(8):

        @pl.when(away(k))
        def _():
            message(k).start()

        @pl.when(jnp.logical_not(away(k)))
        def _():
            q_out[z] = stage[k]

    kv2_ring.forward()
    kv2_ring.near()
    with_partner(kv.at[c, (b + 3) % 4], 5).start()
    with_partner(kv.at[c, (b + 1) % 4], 6).start()
    kv2_ring.far()
    with_partner(kv.at[c, (b + 2) % 4], 7).start()

    for g in range(8):

        @pl.when(jnp.logical_or(g != z, z // 2 != y))
        def _():
            pltpu.make_async_remote_copy(
                src_ref=stage.at[0],
                dst_ref=q_out.at[g],
                send_sem=qsend.at[0],
                recv_sem=qrecv.at[g],
                device_id=dev(g, z // 2, x, c),
                device_id_type=MESH,
            ).wait_recv()

    with_partner(kv.at[o, a], 4).wait_recv()
    with_partner(kv.at[o, (a + 3) % 4], 5).wait_recv()
    with_partner(kv.at[o, (a + 1) % 4], 6).wait_recv()
    with_partner(kv.at[o, (a + 2) % 4], 7).wait_recv()
    for ring in (tok_ring, wts_ring, kv1_ring, kv2_ring):
        ring.drain()
    for d in range(1, 8):
        exchange(d, (z + d) % 8, z).wait_send()
    with_partner(wts.at[x, c], 0).wait_send()
    with_partner(wts.at[(x + 3) % 4, c], 1).wait_send()
    with_partner(wts.at[(x + 1) % 4, c], 2).wait_send()
    with_partner(wts.at[(x + 2) % 4, c], 3).wait_send()
    with_partner(kv.at[c, b], 4).wait_send()
    with_partner(kv.at[c, (b + 3) % 4], 5).wait_send()
    with_partner(kv.at[c, (b + 1) % 4], 6).wait_send()
    with_partner(kv.at[c, (b + 2) % 4], 7).wait_send()
    for k in range(8):

        @pl.when(away(k))
        def _():
            message(k).wait_send()


def prepare(places, tokens, wq, kvw):
    dma = pltpu.SemaphoreType.DMA
    return pl.pallas_call(
        prepare_kernel,
        in_specs=[SMEM, VMEM, VMEM, HBM, HBM, HBM],
        out_specs=[VMEM, VMEM],
        out_shape=[
            jax.ShapeDtypeStruct((8, 64, 256), BF16),
            jax.ShapeDtypeStruct((2, 4, 4, 8, 64, 128), BF16),
        ],
        scratch_shapes=[
            pltpu.VMEM((4, 2, 32, WIDTH), BF16),
            pltpu.VMEM((4, 2, 2, 32, WIDTH), BF16),
            pltpu.VMEM((WIDTH, 1024), BF16),
            pltpu.VMEM((8, 64, 128), BF16),
            pltpu.VMEM((8, 64, 256), BF16),
            pltpu.VMEM((2, 32, 256), F32),
            dma((6,)),
            dma((24,)),
            dma((24,)),
            dma((7,)),
            dma((7,)),
            dma((8,)),
            dma((8,)),
            dma((8,)),
            dma((8,)),
        ],
        compiler_params=pltpu.CompilerParams(collective_id=1, has_side_effects=True),
        name="prepare",
    )(
        places,
        jnp.asarray(np.tile(INVERSE, 4)[None, :]),
        jnp.asarray(np.tile(INVERSE[:, None], (1, 128))),
        tokens.reshape(2, 32, WIDTH),
        wq.T.reshape(2, 32, WIDTH),
        kvw,
    )


def attend_kernel(places, sinks, q_ref, kv_ref, o_ref, order, vt, qt, gap, s):
    z, y, x, c = place()
    offset = (x * 2 + c) * 64
    for b in range(NBLK):
        order[places[b]] = b
    sink = sinks[z * 4 + y] * math.log2(math.e)

    key = lax.broadcasted_iota(I32, (BLK, 256), 0)
    col = lax.broadcasted_iota(I32, (BLK, 256), 1)
    key = ((key >> 6) & 3) * 128 + (key >> 8) * 64 + (key & 63)
    gap[...] = key - ((col >> 6) * BLK + offset + (col & 63))

    def keys_of(i):
        b = order[i]
        g, r = b // 4, b % 4
        return kv_ref[0, r, :, g].reshape(256, 128), kv_ref[1, :, r, g].reshape(256, 128)

    lane = lax.broadcasted_iota(I32, (64, 256), 1)
    zero = jnp.where(lax.broadcasted_iota(I32, (80, 256), 0) < 64, 0.0, 1.0)
    vt[...] = jnp.ones((NBLK, 2, 80, 256), BF16)

    def load_queries(first, slot):
        q = jnp.zeros((64, 256), F32)
        for a in range(4):
            b = order[first + a]
            part = pltpu.roll(q_ref[b // 4].astype(F32), ((a + 4 - b % 4) % 4) * 64, 1)
            q = jnp.where(lane >> 6 == a, part, q)
        qt[slot, :64] = q.astype(BF16)
        qt[slot, 64:] = jnp.zeros((64, 256), BF16)

    def raw_scores(i, slot):
        return [dot(keys, qt[slot], 1, 0) for keys in keys_of(i)]

    def keep(raw, limit, store):
        peaks = []
        for part, scores in enumerate(raw):
            rows = pl.ds(256 * part, 256)
            scores = scores * SCALE_LOG2
            if limit is not None:
                scores = jnp.where(gap[rows] <= limit, scores, NEG)
            store[rows] = scores
            peaks.append(jnp.max(scores, axis=0, keepdims=True))
        return jnp.maximum(*peaks)

    def weigh(i, store, m, acc):
        for part in range(2):
            w = jnp.exp2(store[256 * part : 256 * part + 256] - m).astype(BF16)
            acc = acc + dot(vt[i, part], w, 1, 0)
        return acc

    def step(i, states):
        raw = [raw_scores(i + 1, slot) for slot in range(2)]
        done = []
        for slot in range(2):
            m, acc, peak = states[slot]
            new = jnp.maximum(m, peak)
            acc = weigh(i, s.at[slot], new, acc * jnp.exp2(m - new))
            done.append((new, acc, keep(raw[slot], None, s.at[slot])))
        return tuple(done)

    def finish(first, acc):
        out = acc[:64] / acc[64:65]
        out = jnp.concatenate([out, jnp.zeros((64, 256), F32)], axis=0).T
        for a in range(4):
            top, low = out[64 * a : 64 * a + 32], out[64 * a + 32 : 64 * a + 64]
            o_ref[order[first + a]] = (top + pltpu.roll(low, 64, 1)).astype(BF16)

    def tiles(j, _):
        base = 8 * j
        for slot in range(2):
            load_queries(base + 4 * slot, slot)
        def turn(i):
            for part, keys in enumerate(keys_of(i)):
                vt[i, part, :64] = keys.T[64:]

        def three(u):
            first = jnp.where(u == 4, 0, base + u)
            last = jnp.where(u == 4, 0, base + 4 + u)
            limit = jnp.where(u == 4, 32 * BLK, -u * BLK)
            raw = raw_scores(first, 0), raw_scores(first, 1), raw_scores(last, 1)
            return raw, (limit, None, limit)

        def keep_three(raw, limits):
            return tuple(keep(raw[n], limits[n], s.at[n]) for n in range(3))

        def near(u, carry):
            (m0, acc0), (m1, acc1), (p0, p1, p2) = carry
            raw, limits = three(u + 1)
            turn(base + u)
            turn(base + 4 + u)
            n0 = jnp.maximum(m0, p0)
            n1 = jnp.maximum(m1, jnp.maximum(p1, p2))
            acc0 = weigh(base + u, s.at[0], n0, acc0 * jnp.exp2(m0 - n0))
            acc1 = weigh(base + u, s.at[1], n1, acc1 * jnp.exp2(m1 - n1))
            acc1 = weigh(base + 4 + u, s.at[2], n1, acc1)
            return (n0, acc0), (n1, acc1), keep_three(raw, limits)

        m = jnp.full((1, 256), sink, F32)
        carry = (m, zero), (m, zero), keep_three(*three(0))
        carry = lax.fori_loop(0, 2, lambda t, v: near(2 * t + 1, near(2 * t, v)), carry)
        states = tuple((*carry[slot], carry[2][slot]) for slot in range(2))

        def pair(t, states):
            return step(2 * t + 1, step(2 * t, states))

        states = lax.fori_loop(0, 4 * j, pair, states)
        for slot in range(2):
            finish(base + 4 * slot, states[slot][1])
        return 0

    lax.fori_loop(0, NBLK // 8, tiles, 0)


def attend(places, sinks, q, kv):
    return pl.pallas_call(
        attend_kernel,
        in_specs=[SMEM, SMEM, VMEM, VMEM],
        out_specs=VMEM,
        out_shape=jax.ShapeDtypeStruct((NBLK, 32, 128), BF16),
        scratch_shapes=[
            pltpu.SMEM((NBLK,), I32),
            pltpu.VMEM((NBLK, 2, 80, 256), BF16),
            pltpu.VMEM((2, 128, 256), BF16),
            pltpu.VMEM((BLK, 256), I32),
            pltpu.VMEM((3, BLK, 256), F32),
        ],
        name="attend",
    )(places, sinks, q, kv)


def return_kernel(o_hbm, out, held, own, lsem, send, recv):
    z, y, x, c = place()
    local = [
        pltpu.make_async_copy(o_hbm, own, lsem.at[0]),
        pltpu.make_async_copy(o_hbm.at[z * 4 + y], held.at[z * 4 + y], lsem.at[1]),
    ]
    for copy in local:
        copy.start()
    barrier_with([dev((z + dz) % 8, (y + dy) % 4, x, c) for dz, dy in OFFSETS])
    for copy in local:
        copy.wait()
    copies = []
    for k, (dz, dy) in enumerate(OFFSETS):
        zz, yy = (z + dz) % 8, (y + dy) % 4
        copy = pltpu.make_async_remote_copy(
            src_ref=own.at[zz * 4 + yy],
            dst_ref=held.at[z * 4 + y],
            send_sem=send.at[k],
            recv_sem=recv.at[k],
            device_id=dev(zz, yy, x, c),
            device_id_type=MESH,
        )
        copy.start()
        copies.append(copy)
    for k, (dz, dy) in enumerate(OFFSETS):
        zz, yy = (z + 8 - dz) % 8, (y + 4 - dy) % 4
        pltpu.make_async_remote_copy(
            src_ref=own.at[0],
            dst_ref=held.at[zz * 4 + yy],
            send_sem=send.at[k],
            recv_sem=recv.at[k],
            device_id=dev(zz, yy, x, c),
            device_id_type=MESH,
        ).wait_recv()
    lane = lax.broadcasted_iota(I32, (32, 128), 1)
    for k in range(16):
        p, q = held[2 * k].astype(F32), held[2 * k + 1].astype(F32)
        cols = pl.ds(128 * k, 128)
        out[:32, cols] = jnp.where(lane < 64, p, pltpu.roll(q, 64, 1)).astype(BF16)
        out[32:, cols] = jnp.where(lane < 64, pltpu.roll(p, 64, 1), q).astype(BF16)
    for copy in copies:
        copy.wait_send()


def send_back(o):
    return pl.pallas_call(
        return_kernel,
        in_specs=[HBM],
        out_specs=VMEM,
        out_shape=jax.ShapeDtypeStruct((64, 2048), BF16),
        scratch_shapes=[
            pltpu.VMEM((NBLK, 32, 128), BF16),
            pltpu.VMEM((NBLK, 32, 128), BF16),
            pltpu.SemaphoreType.DMA((2,)),
            pltpu.SemaphoreType.DMA((31,)),
            pltpu.SemaphoreType.DMA((31,)),
        ],
        compiler_params=pltpu.CompilerParams(collective_id=3, has_side_effects=True),
        name="send_back",
    )(o)


def per_device(tokens, query_weight, key_value_weight, block_places, sinks):
    q, kv = prepare(block_places, tokens, query_weight, key_value_weight)
    o = attend(block_places, sinks, q, kv)
    return send_back(o)


def solution(mesh):
    in_specs = (P(("grp", "sp"), None), P(None, "sp"), P(), P(), P())
    return jax.shard_map(
        per_device,
        mesh=mesh,
        in_specs=in_specs,
        out_specs=P(("grp", "sp"), None),
        check_vma=False,
    )
```

```python
import math

import jax
import jax.numpy as jnp
import numpy as np
from jax import lax
from jax.experimental import pallas as pl
from jax.experimental.pallas import tpu as pltpu
from jax.sharding import PartitionSpec as P

MESH = pl.DeviceIdType.MESH
BF16, F32, I32 = jnp.bfloat16, jnp.float32, jnp.int32
WIDTH = 2880
HEAD = 64
BLK = 512
NBLK = 32
SCALE_LOG2 = HEAD**-0.5 * math.log2(math.e)
NEG = -1e30
VMEM = pl.BlockSpec(memory_space=pltpu.VMEM)
HBM = pl.BlockSpec(memory_space=pltpu.HBM)
SMEM = pl.BlockSpec(memory_space=pltpu.SMEM)
OFFSETS = [(dz, dy) for dz in range(8) for dy in range(4) if dz or dy]
INVERSE = (150000.0 ** (-(np.arange(32, dtype=np.float64) * 2.0) / HEAD)).astype(np.float32)


def place():
    z = lax.axis_index("grp")
    s = lax.axis_index("sp")
    return z, s // 8, (s // 2) % 4, s % 2


def dev(z, y, x, c):
    return (z, (y * 4 + x) * 2 + c)


def dot(a, b, ca, cb):
    return lax.dot_general(a, b, (((ca,), (cb,)), ((), ())), preferred_element_type=F32)


class Ring:
    def __init__(self, at, me, right, left, send, recv, first):
        self.at, self.me, self.right, self.left = at, me, right, left
        self.send, self.recv, self.first = send, recv, first
        self.prev, self.next, self.opp = (me + 3) % 4, (me + 1) % 4, (me + 2) % 4

    def copy(self, piece, half, target, k):
        ref = self.at(piece, half)
        return pltpu.make_async_remote_copy(
            src_ref=ref,
            dst_ref=ref,
            send_sem=self.send.at[self.first + k],
            recv_sem=self.recv.at[self.first + k],
            device_id=target,
            device_id_type=MESH,
        )

    def start(self):
        self.copy(self.me, 0, self.right, 0).start()
        self.copy(self.me, 1, self.left, 2).start()
        self.copy(self.me, 1, self.right, 1).start()
        self.copy(self.me, 0, self.left, 3).start()

    def forward(self):
        self.copy(self.prev, 0, self.right, 0).wait_recv()
        self.copy(self.prev, 0, self.right, 4).start()
        self.copy(self.next, 1, self.left, 2).wait_recv()
        self.copy(self.next, 1, self.left, 5).start()

    def near(self):
        self.copy(self.prev, 1, self.right, 1).wait_recv()
        self.copy(self.next, 0, self.left, 3).wait_recv()

    def far(self):
        self.copy(self.opp, 0, self.right, 4).wait_recv()
        self.copy(self.opp, 1, self.left, 5).wait_recv()

    def drain(self):
        self.copy(self.me, 0, self.right, 0).wait_send()
        self.copy(self.me, 1, self.right, 1).wait_send()
        self.copy(self.me, 1, self.left, 2).wait_send()
        self.copy(self.me, 0, self.left, 3).wait_send()
        self.copy(self.prev, 0, self.right, 4).wait_send()
        self.copy(self.next, 1, self.left, 5).wait_send()


def prepare_part(
    places, inv_row, inv_col, tok_hbm, wqt_hbm, kvw_hbm, q_out, kv, order,
    tok, wts, kvw, kvp, stage, angles, lsem, send, recv, zsend, zrecv, psend, precv, qsend, qrecv,
):
    z, y, x, c = place()
    o = 1 - c
    a, b = x * o + y * c, y * o + x * c
    partner = dev(z, y, x, o)
    ring_y = (dev(z, (y + 1) % 4, x, c), dev(z, (y + 3) % 4, x, c))
    ring_x = (dev(z, y, (x + 1) % 4, c), dev(z, y, (x + 3) % 4, c))
    others = [dev((z + d) % 8, y, x, c) for d in range(1, 8)]
    peers = [dev((z + dz) % 8, (y + dy) % 4, x, c) for dz, dy in OFFSETS]
    peers += [*ring_x, partner]

    ready = pltpu.get_barrier_semaphore()
    for peer in peers:
        pl.semaphore_signal(ready, inc=1, device_id=peer, device_id_type=MESH)

    own = [
        pltpu.make_async_copy(tok_hbm, tok.at[y], lsem.at[0]),
        pltpu.make_async_copy(wqt_hbm, wts.at[x, c], lsem.at[1]),
    ]
    for n in range(4):
        cols = pl.ds(256 * n, 256)
        own.append(pltpu.make_async_copy(kvw_hbm.at[:, cols], kvw.at[:, cols], lsem.at[2 + n]))
    for n in (0, 1, 2, 4, 3, 5):
        own[n].start()

    lane = lax.broadcasted_iota(I32, (64, 128), 1)
    base = places[z * 4 + y] * BLK + (x * 2 + c) * 64
    angle = (base + lax.broadcasted_iota(I32, (64, 128), 0)).astype(F32) * inv_row[...]
    cosine = jnp.cos(angle)
    sine = jnp.where(lane % 64 < 32, -1.0, 1.0) * jnp.sin(angle)
    own[0].wait()
    own[1].wait()
    pl.semaphore_wait(ready, len(peers))

    tok_ring = Ring(lambda p, h: tok.at[p, h], y, *ring_y, send, recv, 0)
    wts_ring = Ring(lambda p, h: wts.at[p, c, h], x, *ring_x, send, recv, 6)
    near = [
        dev(z, (y + c) % 4, (x + o) % 4, c),
        dev(z, (y + 3 * c) % 4, (x + 3 * o) % 4, c),
    ]
    wide = [
        dev(z, (y + o) % 4, (x + c) % 4, c),
        dev(z, (y + 3 * o) % 4, (x + 3 * c) % 4, c),
    ]
    kv1_ring = Ring(lambda p, h: kv.at[c, b, p, pl.ds(4 * h, 4)], a, *near, send, recv, 12)
    kv2_ring = Ring(lambda p, h: kv.at[c, p, :, pl.ds(4 * h, 4)], b, *wide, send, recv, 18)

    def with_partner(ref, k):
        return pltpu.make_async_remote_copy(
            src_ref=ref,
            dst_ref=ref,
            send_sem=psend.at[k],
            recv_sem=precv.at[k],
            device_id=partner,
            device_id_type=MESH,
        )

    def exchange(d, head, source):
        return pltpu.make_async_remote_copy(
            src_ref=kvp.at[head],
            dst_ref=kv.at[c, b, a, source],
            send_sem=zsend.at[d - 1],
            recv_sem=zrecv.at[d - 1],
            device_id=others[d - 1],
            device_id_type=MESH,
        )

    tok_ring.start()
    wts_ring.start()
    with_partner(wts.at[x, c], 0).start()

    rows = tok[y].reshape(64, WIDTH)
    for n in range(2):
        own[2 + n].wait()
        own[4 + n].wait()
        keys = jnp.dot(rows, kvw[:, 256 * n : 256 * n + 256], preferred_element_type=F32)
        values = jnp.dot(rows, kvw[:, 512 + 256 * n : 768 + 256 * n], preferred_element_type=F32)
        for p in range(2):
            k, v = keys[:, 128 * p : 128 * p + 128], values[:, 128 * p : 128 * p + 128]
            swapped = jnp.where(lane % 64 < 32, pltpu.roll(k, 96, 1), pltpu.roll(k, 32, 1))
            k = k * cosine + swapped * sine
            kvp[4 * n + 2 * p] = jnp.where(lane < 64, k, pltpu.roll(v, 64, 1)).astype(BF16)
            kvp[4 * n + 2 * p + 1] = jnp.where(lane < 64, pltpu.roll(k, 64, 1), v).astype(BF16)
    kv[c, b, a, z] = kvp[z]

    for d in range(1, 8):
        exchange(d, (z + d) % 8, z).start()

    col = lax.broadcasted_iota(I32, (32, 256), 1)
    block = jnp.where(
        col < 128,
        jnp.where(col < 64, places[z * 4], places[z * 4 + 1]),
        jnp.where(col < 192, places[z * 4 + 2], places[z * 4 + 3]),
    )
    angle = (block * BLK + (x * 2 + c) * 64 + col % 64).astype(F32)
    angle = angle * jnp.concatenate([inv_col[...], inv_col[...]], axis=1)
    angles[0], angles[1] = jnp.cos(angle), jnp.sin(angle)
    def place_block(i, _):
        found = 0
        for n in range(NBLK):
            found = jnp.where(places[n] == i, n, found)
        order[i] = found
        return 0

    lax.fori_loop(0, NBLK, place_block, 0)
    for d in range(1, 8):
        exchange(d, z, (z + 8 - d) % 8).wait_recv()
    kv1_ring.start()

    wts_ring.forward()
    tok_ring.forward()
    wts_ring.near()
    with_partner(wts.at[(x + 3) % 4, c], 1).start()
    with_partner(wts.at[(x + 1) % 4, c], 2).start()
    tok_ring.near()
    kv1_ring.forward()
    wts_ring.far()
    with_partner(wts.at[(x + 2) % 4, c], 3).start()
    kv1_ring.near()
    kv1_ring.far()
    kv2_ring.start()
    with_partner(kv.at[c, b], 4).start()
    tok_ring.far()
    with_partner(wts.at[x, o], 0).wait_recv()
    with_partner(wts.at[(x + 3) % 4, o], 1).wait_recv()
    with_partner(wts.at[(x + 1) % 4, o], 2).wait_recv()
    with_partner(wts.at[(x + 2) % 4, o], 3).wait_recv()

    def message(k):
        return pltpu.make_async_remote_copy(
            src_ref=stage.at[k],
            dst_ref=q_out.at[z],
            send_sem=qsend.at[k],
            recv_sem=qrecv.at[z],
            device_id=dev(2 * y + k // 4, k % 4, x, c),
            device_id_type=MESH,
        )

    def away(k):
        return jnp.logical_or(2 * y + k // 4 != z, k % 4 != y)

    rows = tok[...].reshape(256, WIDTH)
    for half in range(2):
        w = wts[2 * half : 2 * half + 2].reshape(256, WIDTH)
        q = dot(w, rows, 1, 1)
        for i in range(4):
            k = half * 4 + i
            lo, hi = q[i * 64 : i * 64 + 32], q[i * 64 + 32 : i * 64 + 64]
            stage[k, :32] = (lo * angles[0] - hi * angles[1]).astype(BF16)
            stage[k, 32:] = (hi * angles[0] + lo * angles[1]).astype(BF16)
    for k in range(8):

        @pl.when(away(k))
        def _():
            message(k).start()

        @pl.when(jnp.logical_not(away(k)))
        def _():
            q_out[z] = stage[k]

    kv2_ring.forward()
    kv2_ring.near()
    with_partner(kv.at[c, (b + 3) % 4], 5).start()
    with_partner(kv.at[c, (b + 1) % 4], 6).start()
    kv2_ring.far()
    with_partner(kv.at[c, (b + 2) % 4], 7).start()

    for g in range(8):

        @pl.when(jnp.logical_or(g != z, z // 2 != y))
        def _():
            pltpu.make_async_remote_copy(
                src_ref=stage.at[0],
                dst_ref=q_out.at[g],
                send_sem=qsend.at[0],
                recv_sem=qrecv.at[g],
                device_id=dev(g, z // 2, x, c),
                device_id_type=MESH,
            ).wait_recv()

    with_partner(kv.at[o, a], 4).wait_recv()
    with_partner(kv.at[o, (a + 3) % 4], 5).wait_recv()
    with_partner(kv.at[o, (a + 1) % 4], 6).wait_recv()
    with_partner(kv.at[o, (a + 2) % 4], 7).wait_recv()
    for ring in (tok_ring, wts_ring, kv1_ring, kv2_ring):
        ring.drain()
    for d in range(1, 8):
        exchange(d, (z + d) % 8, z).wait_send()
    with_partner(wts.at[x, c], 0).wait_send()
    with_partner(wts.at[(x + 3) % 4, c], 1).wait_send()
    with_partner(wts.at[(x + 1) % 4, c], 2).wait_send()
    with_partner(wts.at[(x + 2) % 4, c], 3).wait_send()
    with_partner(kv.at[c, b], 4).wait_send()
    with_partner(kv.at[c, (b + 3) % 4], 5).wait_send()
    with_partner(kv.at[c, (b + 1) % 4], 6).wait_send()
    with_partner(kv.at[c, (b + 2) % 4], 7).wait_send()
    for k in range(8):

        @pl.when(away(k))
        def _():
            message(k).wait_send()


def attend_part(sinks, q_ref, kv_ref, o_ref, order, vt, qt, gap, s):
    z, y, x, c = place()
    offset = (x * 2 + c) * 64
    sink = sinks[z * 4 + y] * math.log2(math.e)

    key = lax.broadcasted_iota(I32, (BLK, 256), 0)
    col = lax.broadcasted_iota(I32, (BLK, 256), 1)
    key = ((key >> 6) & 3) * 128 + (key >> 8) * 64 + (key & 63)
    gap[...] = key - ((col >> 6) * BLK + offset + (col & 63))

    def keys_of(i):
        b = order[i]
        g, r = b // 4, b % 4
        return kv_ref[0, r, :, g].reshape(256, 128), kv_ref[1, :, r, g].reshape(256, 128)

    lane = lax.broadcasted_iota(I32, (64, 128), 1)
    zero = jnp.where(lax.broadcasted_iota(I32, (80, 256), 0) < 64, 0.0, 1.0)
    vt[...] = jnp.ones((NBLK, 2, 80, 256), BF16)

    def load_queries(first, slot):
        for half in range(2):
            parts = []
            for a in range(2):
                b = order[first + 2 * half + a]
                four = q_ref[b // 4].astype(F32)
                two = jnp.where(b % 4 >= 2, four[:, 128:], four[:, :128])
                parts.append(jnp.where(b % 2 == a, two, pltpu.roll(two, 64, 1)))
            q = jnp.where(lane < 64, *parts)
            qt[slot, :64, 128 * half : 128 * half + 128] = q.astype(BF16)
        qt[slot, 64:] = jnp.zeros((64, 256), BF16)

    def raw_scores(i, slot):
        return [dot(keys, qt[slot], 1, 0) for keys in keys_of(i)]

    def keep(raw, limit, store):
        peaks = []
        for part, scores in enumerate(raw):
            rows = pl.ds(256 * part, 256)
            scores = scores * SCALE_LOG2
            if limit is not None:
                scores = jnp.where(gap[rows] <= limit, scores, NEG)
            store[rows] = scores
            peaks.append(jnp.max(scores, axis=0, keepdims=True))
        return jnp.maximum(*peaks)

    def weigh(i, store, m, acc):
        for part in range(2):
            w = jnp.exp2(store[256 * part : 256 * part + 256] - m).astype(BF16)
            acc = acc + dot(vt[i, part], w, 1, 0)
        return acc

    def step(i, states):
        raw = [raw_scores(i + 1, slot) for slot in range(2)]
        done = []
        for slot in range(2):
            m, acc, peak = states[slot]
            new = jnp.maximum(m, peak)
            acc = weigh(i, s.at[slot], new, acc * jnp.exp2(m - new))
            done.append((new, acc, keep(raw[slot], None, s.at[slot])))
        return tuple(done)

    def finish(first, acc):
        out = acc[:64] / acc[64:65]
        out = jnp.concatenate([out, jnp.zeros((64, 256), F32)], axis=0).T
        for a in range(4):
            top, low = out[64 * a : 64 * a + 32], out[64 * a + 32 : 64 * a + 64]
            o_ref[first + a] = (top + pltpu.roll(low, 64, 1)).astype(BF16)

    def tiles(j, _):
        base = 8 * j
        for slot in range(2):
            load_queries(base + 4 * slot, slot)
        def turn(i):
            for part, keys in enumerate(keys_of(i)):
                vt[i, part, :64] = keys.T[64:]

        def three(u):
            first = jnp.where(u == 4, 0, base + u)
            last = jnp.where(u == 4, 0, base + 4 + u)
            limit = jnp.where(u == 4, 32 * BLK, -u * BLK)
            raw = raw_scores(first, 0), raw_scores(first, 1), raw_scores(last, 1)
            return raw, (limit, None, limit)

        def keep_three(raw, limits):
            return tuple(keep(raw[n], limits[n], s.at[n]) for n in range(3))

        def near(u, carry):
            (m0, acc0), (m1, acc1), (p0, p1, p2) = carry
            raw, limits = three(u + 1)
            turn(base + u)
            turn(base + 4 + u)
            n0 = jnp.maximum(m0, p0)
            n1 = jnp.maximum(m1, jnp.maximum(p1, p2))
            acc0 = weigh(base + u, s.at[0], n0, acc0 * jnp.exp2(m0 - n0))
            acc1 = weigh(base + u, s.at[1], n1, acc1 * jnp.exp2(m1 - n1))
            acc1 = weigh(base + 4 + u, s.at[2], n1, acc1)
            return (n0, acc0), (n1, acc1), keep_three(raw, limits)

        m = jnp.full((1, 256), sink, F32)
        carry = (m, zero), (m, zero), keep_three(*three(0))
        carry = lax.fori_loop(0, 2, lambda t, v: near(2 * t + 1, near(2 * t, v)), carry)
        states = tuple((*carry[slot], carry[2][slot]) for slot in range(2))

        def pair(t, states):
            return step(2 * t + 1, step(2 * t, states))

        states = lax.fori_loop(0, 4 * j, pair, states)
        for slot in range(2):
            finish(base + 4 * slot, states[slot][1])
        return 0

    lax.fori_loop(0, NBLK // 8, tiles, 0)


def return_part(places, o_ref, out, held, own, send, recv):
    z, y, x, c = place()
    for b in range(NBLK):
        own[b] = o_ref[places[b]]
    held[z * 4 + y] = own[z * 4 + y]

    def copy(k, block, head, target):
        return pltpu.make_async_remote_copy(
            src_ref=own.at[block],
            dst_ref=held.at[head],
            send_sem=send.at[k],
            recv_sem=recv.at[k],
            device_id=target,
            device_id_type=MESH,
        )

    def sent(k):
        dz, dy = OFFSETS[k]
        zz, yy = (z + dz) % 8, (y + dy) % 4
        return copy(k, zz * 4 + yy, z * 4 + y, dev(zz, yy, x, c))

    for k in range(31):
        sent(k).start()
    for k, (dz, dy) in enumerate(OFFSETS):
        zz, yy = (z + 8 - dz) % 8, (y + 4 - dy) % 4
        copy(k, 0, zz * 4 + yy, dev(zz, yy, x, c)).wait_recv()
    lane = lax.broadcasted_iota(I32, (32, 128), 1)
    for k in range(16):
        p, q = held[2 * k].astype(F32), held[2 * k + 1].astype(F32)
        cols = pl.ds(128 * k, 128)
        out[:32, cols] = jnp.where(lane < 64, p, pltpu.roll(q, 64, 1)).astype(BF16)
        out[32:, cols] = jnp.where(lane < 64, pltpu.roll(p, 64, 1), q).astype(BF16)
    for k in range(31):
        sent(k).wait_send()


def kernel(
    places, sinks, inv_row, inv_col, tok_hbm, wqt_hbm, kvw_hbm, out,
    q, kv, order, tok, wts, kvw, kvp, stage, angles,
    lsem, send, recv, zsend, zrecv, psend, precv, qsend, qrecv,
    attended, vt, qt, gap, s, held, own, osend, orecv,
):
    prepare_part(
        places, inv_row, inv_col, tok_hbm, wqt_hbm, kvw_hbm, q, kv, order,
        tok, wts, kvw, kvp, stage, angles,
        lsem, send, recv, zsend, zrecv, psend, precv, qsend, qrecv,
    )
    attend_part(sinks, q, kv, attended, order, vt, qt, gap, s)
    return_part(places, attended, out, held, own, osend, orecv)


def per_device(tokens, query_weight, key_value_weight, block_places, sinks):
    dma = pltpu.SemaphoreType.DMA
    return pl.pallas_call(
        kernel,
        in_specs=[SMEM, SMEM, VMEM, VMEM, HBM, HBM, HBM],
        out_specs=VMEM,
        out_shape=jax.ShapeDtypeStruct((64, 2048), BF16),
        scratch_shapes=[
            pltpu.VMEM((8, 64, 256), BF16),
            pltpu.VMEM((2, 4, 4, 8, 64, 128), BF16),
            pltpu.SMEM((NBLK,), I32),
            pltpu.VMEM((4, 2, 32, WIDTH), BF16),
            pltpu.VMEM((4, 2, 2, 32, WIDTH), BF16),
            pltpu.VMEM((WIDTH, 1024), BF16),
            pltpu.VMEM((8, 64, 128), BF16),
            pltpu.VMEM((8, 64, 256), BF16),
            pltpu.VMEM((2, 32, 256), F32),
            dma((6,)),
            dma((24,)),
            dma((24,)),
            dma((7,)),
            dma((7,)),
            dma((8,)),
            dma((8,)),
            dma((8,)),
            dma((8,)),
            pltpu.VMEM((NBLK, 32, 128), BF16),
            pltpu.VMEM((NBLK, 2, 80, 256), BF16),
            pltpu.VMEM((2, 128, 256), BF16),
            pltpu.VMEM((BLK, 256), I32),
            pltpu.VMEM((3, BLK, 256), F32),
            pltpu.VMEM((NBLK, 32, 128), BF16),
            pltpu.VMEM((NBLK, 32, 128), BF16),
            dma((31,)),
            dma((31,)),
        ],
        compiler_params=pltpu.CompilerParams(collective_id=1, has_side_effects=True),
        name="layer",
    )(
        block_places,
        sinks,
        jnp.asarray(np.tile(INVERSE, 4)[None, :]),
        jnp.asarray(np.tile(INVERSE[:, None], (1, 128))),
        tokens.reshape(2, 32, WIDTH),
        query_weight.T.reshape(2, 32, WIDTH),
        key_value_weight,
    )


def solution(mesh):
    in_specs = (P(("grp", "sp"), None), P(None, "sp"), P(), P(), P())
    return jax.shard_map(
        per_device,
        mesh=mesh,
        in_specs=in_specs,
        out_specs=P(("grp", "sp"), None),
        check_vma=False,
    )
```

```python
import math

import jax
import jax.numpy as jnp
import numpy as np
from jax import lax
from jax.experimental import pallas as pl
from jax.experimental.pallas import tpu as pltpu
from jax.sharding import PartitionSpec as P

MESH = pl.DeviceIdType.MESH
BF16, F32, I32 = jnp.bfloat16, jnp.float32, jnp.int32
WIDTH = 2880
HEAD = 64
BLK = 512
NBLK = 32
SCALE_LOG2 = HEAD**-0.5 * math.log2(math.e)
NEG = -1e30
VMEM = pl.BlockSpec(memory_space=pltpu.VMEM)
HBM = pl.BlockSpec(memory_space=pltpu.HBM)
SMEM = pl.BlockSpec(memory_space=pltpu.SMEM)
OFFSETS = [(dz, dy) for dz in range(8) for dy in range(4) if dz or dy]
INVERSE = (150000.0 ** (-(np.arange(32, dtype=np.float64) * 2.0) / HEAD)).astype(np.float32)


def place():
    z = lax.axis_index("grp")
    s = lax.axis_index("sp")
    return z, s // 8, (s // 2) % 4, s % 2


def dev(z, y, x, c):
    return (z, (y * 4 + x) * 2 + c)


def dot(a, b, ca, cb):
    return lax.dot_general(a, b, (((ca,), (cb,)), ((), ())), preferred_element_type=F32)


class Ring:
    def __init__(self, at, me, right, left, send, recv, first):
        self.at, self.me, self.right, self.left = at, me, right, left
        self.send, self.recv, self.first = send, recv, first
        self.prev, self.next, self.opp = (me + 3) % 4, (me + 1) % 4, (me + 2) % 4

    def copy(self, piece, half, target, k):
        ref = self.at(piece, half)
        return pltpu.make_async_remote_copy(
            src_ref=ref,
            dst_ref=ref,
            send_sem=self.send.at[self.first + k],
            recv_sem=self.recv.at[self.first + k],
            device_id=target,
            device_id_type=MESH,
        )

    def start(self):
        self.copy(self.me, 0, self.right, 0).start()
        self.copy(self.me, 1, self.left, 2).start()
        self.copy(self.me, 1, self.right, 1).start()
        self.copy(self.me, 0, self.left, 3).start()

    def forward(self):
        self.copy(self.prev, 0, self.right, 0).wait_recv()
        self.copy(self.prev, 0, self.right, 4).start()
        self.copy(self.next, 1, self.left, 2).wait_recv()
        self.copy(self.next, 1, self.left, 5).start()

    def near(self):
        self.copy(self.prev, 1, self.right, 1).wait_recv()
        self.copy(self.next, 0, self.left, 3).wait_recv()

    def far(self):
        self.copy(self.opp, 0, self.right, 4).wait_recv()
        self.copy(self.opp, 1, self.left, 5).wait_recv()

    def drain(self):
        self.copy(self.me, 0, self.right, 0).wait_send()
        self.copy(self.me, 1, self.right, 1).wait_send()
        self.copy(self.me, 1, self.left, 2).wait_send()
        self.copy(self.me, 0, self.left, 3).wait_send()
        self.copy(self.prev, 0, self.right, 4).wait_send()
        self.copy(self.next, 1, self.left, 5).wait_send()


def prepare_part(
    places, inv_row, inv_col, tok_hbm, wqt_hbm, kvw_hbm, q_out, kv, order,
    tok, wts, kvw, kvp, stage, mid, angles, lsem, send, recv, zsend, zrecv, psend, precv, ysend, yrecv, qsend, qrecv, known,
):
    z, y, x, c = place()
    o = 1 - c
    a, b = x * o + y * c, y * o + x * c
    partner = dev(z, y, x, o)
    ring_y = (dev(z, (y + 1) % 4, x, c), dev(z, (y + 3) % 4, x, c))
    ring_x = (dev(z, y, (x + 1) % 4, c), dev(z, y, (x + 3) % 4, c))
    others = [dev((z + d) % 8, y, x, c) for d in range(1, 8)]
    ring_z = (others[0], others[6])
    peers = [*ring_y, *ring_x, *ring_z, partner]

    def tell(targets, k):
        for target in targets:
            pl.semaphore_signal(known.at[k], inc=1, device_id=target, device_id_type=MESH)

    def hear(targets, k):
        pl.semaphore_wait(known.at[k], len(targets))

    ready = pltpu.get_barrier_semaphore()
    for peer in peers:
        pl.semaphore_signal(ready, inc=1, device_id=peer, device_id_type=MESH)

    own = [
        pltpu.make_async_copy(tok_hbm, tok.at[y], lsem.at[0]),
        pltpu.make_async_copy(wqt_hbm, wts.at[x, c], lsem.at[1]),
    ]
    for n in range(4):
        cols = pl.ds(256 * n, 256)
        own.append(pltpu.make_async_copy(kvw_hbm.at[:, cols], kvw.at[:, cols], lsem.at[2 + n]))
    for n in (0, 1, 2, 4, 3, 5):
        own[n].start()

    lane = lax.broadcasted_iota(I32, (64, 128), 1)
    base = places[z * 4 + y] * BLK + (x * 2 + c) * 64
    angle = (base + lax.broadcasted_iota(I32, (64, 128), 0)).astype(F32) * inv_row[...]
    cosine = jnp.cos(angle)
    sine = jnp.where(lane % 64 < 32, -1.0, 1.0) * jnp.sin(angle)
    own[0].wait()
    own[1].wait()
    pl.semaphore_wait(ready, len(peers))

    tok_ring = Ring(lambda p, h: tok.at[p, h], y, *ring_y, send, recv, 0)
    wts_ring = Ring(lambda p, h: wts.at[p, c, h], x, *ring_x, send, recv, 6)
    near = [
        dev(z, (y + c) % 4, (x + o) % 4, c),
        dev(z, (y + 3 * c) % 4, (x + 3 * o) % 4, c),
    ]
    wide = [
        dev(z, (y + o) % 4, (x + c) % 4, c),
        dev(z, (y + 3 * o) % 4, (x + 3 * c) % 4, c),
    ]
    kv1_ring = Ring(lambda p, h: kv.at[c, b, p, pl.ds(4 * h, 4)], a, *near, send, recv, 12)
    kv2_rings = [
        Ring(
            lambda p, h, piece=(a + d) % 4: kv.at[c, p, piece, pl.ds(4 * h, 4)],
            b, *wide, send, recv, 18 + 6 * d,
        )
        for d in range(4)
    ]

    def with_partner(ref, k):
        return pltpu.make_async_remote_copy(
            src_ref=ref,
            dst_ref=ref,
            send_sem=psend.at[k],
            recv_sem=precv.at[k],
            device_id=partner,
            device_id_type=MESH,
        )

    def piece(n, p):
        return with_partner(kv.at[c, (b + n) % 4, (a + p) % 4], 4 + 4 * n + p)

    def exchange(d, head, source):
        return pltpu.make_async_remote_copy(
            src_ref=kvp.at[head],
            dst_ref=kv.at[c, b, a, source],
            send_sem=zsend.at[d - 1],
            recv_sem=zrecv.at[d - 1],
            device_id=others[d - 1],
            device_id_type=MESH,
        )

    tok_ring.start()
    wts_ring.start()
    with_partner(wts.at[x, c], 0).start()
    tell(ring_z, 0)
    tell(ring_y, 1)

    rows = tok[y].reshape(64, WIDTH)
    for n in range(2):
        own[2 + n].wait()
        own[4 + n].wait()
        keys = jnp.dot(rows, kvw[:, 256 * n : 256 * n + 256], preferred_element_type=F32)
        values = jnp.dot(rows, kvw[:, 512 + 256 * n : 768 + 256 * n], preferred_element_type=F32)
        for p in range(2):
            k, v = keys[:, 128 * p : 128 * p + 128], values[:, 128 * p : 128 * p + 128]
            swapped = jnp.where(lane % 64 < 32, pltpu.roll(k, 96, 1), pltpu.roll(k, 32, 1))
            k = k * cosine + swapped * sine
            kvp[4 * n + 2 * p] = jnp.where(lane < 64, k, pltpu.roll(v, 64, 1)).astype(BF16)
            kvp[4 * n + 2 * p + 1] = jnp.where(lane < 64, pltpu.roll(k, 64, 1), v).astype(BF16)
    kv[c, b, a, z] = kvp[z]
    hear(ring_z, 0)
    far_z = (others[1], others[5])
    tell(far_z, 2)
    hear(ring_y, 1)
    hear(far_z, 2)
    all_y = [dev(z, (y + d) % 4, x, c) for d in (1, 2, 3)]
    tell(all_y, 3)

    for d in range(1, 8):
        exchange(d, (z + d) % 8, z).start()

    col = lax.broadcasted_iota(I32, (32, 256), 1)
    block = jnp.where(
        col < 128,
        jnp.where(col < 64, places[z * 4], places[z * 4 + 1]),
        jnp.where(col < 192, places[z * 4 + 2], places[z * 4 + 3]),
    )
    angle = (block * BLK + (x * 2 + c) * 64 + col % 64).astype(F32)
    angle = angle * jnp.concatenate([inv_col[...], inv_col[...]], axis=1)
    angles[0], angles[1] = jnp.cos(angle), jnp.sin(angle)
    def place_block(i, _):
        found = 0
        for n in range(NBLK):
            found = jnp.where(places[n] == i, n, found)
        order[i] = found
        return 0

    lax.fori_loop(0, NBLK, place_block, 0)
    for d in range(1, 8):
        exchange(d, z, (z + 8 - d) % 8).wait_recv()
    kv1_ring.start()
    kv2_rings[0].start()
    wts_ring.forward()
    tok_ring.forward()
    wts_ring.near()
    with_partner(wts.at[(x + 3) % 4, c], 1).start()
    with_partner(wts.at[(x + 1) % 4, c], 2).start()
    tok_ring.near()
    kv1_ring.forward()
    kv2_rings[0].forward()
    kv1_ring.near()
    kv2_rings[1].start()
    kv2_rings[3].start()
    wts_ring.far()
    with_partner(wts.at[(x + 2) % 4, c], 3).start()
    tok_ring.far()
    with_partner(wts.at[x, o], 0).wait_recv()
    with_partner(wts.at[(x + 3) % 4, o], 1).wait_recv()
    with_partner(wts.at[(x + 1) % 4, o], 2).wait_recv()
    with_partner(wts.at[(x + 2) % 4, o], 3).wait_recv()

    hear(all_y, 3)
    def along_y(d, half, target, source):
        return pltpu.make_async_remote_copy(
            src_ref=stage.at[target, half],
            dst_ref=mid.at[2 * source + half],
            send_sem=ysend.at[2 * d + half],
            recv_sem=yrecv.at[2 * d + half],
            device_id=dev(z, (y + d) % 4, x, c),
            device_id_type=MESH,
        )

    def along_z(d, half):
        plane = 2 * ((y + 4 - d) % 4) + half
        return plane, pltpu.make_async_remote_copy(
            src_ref=mid.at[plane],
            dst_ref=q_out.at[z],
            send_sem=qsend.at[2 * d + half],
            recv_sem=qrecv.at[z],
            device_id=dev(plane, y, x, c),
            device_id_type=MESH,
        )

    def pass_on(d, half):
        plane, copy = along_z(d, half)

        @pl.when(plane != z)
        def _():
            copy.start()

        @pl.when(plane == z)
        def _():
            q_out[z] = mid[plane]

    rows = tok[...].reshape(256, WIDTH)
    for half in range(2):
        w = wts[2 * half : 2 * half + 2].reshape(256, WIDTH)
        q = dot(w, rows, 1, 1)
        for i in range(4):
            lo, hi = q[i * 64 : i * 64 + 32], q[i * 64 + 32 : i * 64 + 64]
            stage[i, half, :32] = (lo * angles[0] - hi * angles[1]).astype(BF16)
            stage[i, half, 32:] = (hi * angles[0] + lo * angles[1]).astype(BF16)
        for d in (2, 1, 3):
            along_y(d, half, (y + d) % 4, y).start()
        mid[2 * y + half] = stage[y, half]
    for half in range(2):
        pass_on(0, half)

    kv1_ring.far()
    kv2_rings[2].start()
    for p in range(4):
        piece(0, p).start()
    kv2_rings[1].forward()
    kv2_rings[3].forward()

    for half in range(2):
        for d in (1, 3, 2):
            along_y(d, half, y, (y + 4 - d) % 4).wait_recv()
            pass_on(d, half)

    kv2_rings[2].forward()
    for p in (0, 1, 3, 2):
        kv2_rings[p].near()
        piece(1, p).start()
        piece(3, p).start()
    for p in (0, 1, 3, 2):
        kv2_rings[p].far()
        piece(2, p).start()

    for g in range(8):

        @pl.when(g != z)
        def _():
            pltpu.make_async_remote_copy(
                src_ref=mid.at[0],
                dst_ref=q_out.at[g],
                send_sem=qsend.at[0],
                recv_sem=qrecv.at[g],
                device_id=dev(g, y, x, c),
                device_id_type=MESH,
            ).wait_recv()

    for n in range(4):
        for p in range(4):
            with_partner(kv.at[o, (a + n) % 4, (b + p) % 4], 4 + 4 * n + p).wait_recv()
    for ring in (tok_ring, wts_ring, kv1_ring, *kv2_rings):
        ring.drain()
    for d in range(1, 8):
        exchange(d, (z + d) % 8, z).wait_send()
    for half in range(2):
        for d in range(1, 4):
            along_y(d, half, (y + d) % 4, y).wait_send()
        for d in range(4):
            plane, copy = along_z(d, half)

            @pl.when(plane != z)
            def _():
                copy.wait_send()

    with_partner(wts.at[x, c], 0).wait_send()
    with_partner(wts.at[(x + 3) % 4, c], 1).wait_send()
    with_partner(wts.at[(x + 1) % 4, c], 2).wait_send()
    with_partner(wts.at[(x + 2) % 4, c], 3).wait_send()
    for n in range(4):
        for p in range(4):
            piece(n, p).wait_send()


def attend_part(sinks, q_ref, kv_ref, o_ref, order, vt, qt, gap, s):
    z, y, x, c = place()
    offset = (x * 2 + c) * 64
    sink = sinks[z * 4 + y] * math.log2(math.e)

    key = lax.broadcasted_iota(I32, (BLK, 256), 0)
    col = lax.broadcasted_iota(I32, (BLK, 256), 1)
    key = ((key >> 6) & 3) * 128 + (key >> 8) * 64 + (key & 63)
    gap[...] = key - ((col >> 6) * BLK + offset + (col & 63))

    def keys_of(i):
        b = order[i]
        g, r = b // 4, b % 4
        return kv_ref[0, r, :, g].reshape(256, 128), kv_ref[1, :, r, g].reshape(256, 128)

    lane = lax.broadcasted_iota(I32, (64, 128), 1)
    zero = jnp.where(lax.broadcasted_iota(I32, (80, 256), 0) < 64, 0.0, 1.0)
    vt[...] = jnp.ones((NBLK, 2, 80, 256), BF16)

    def load_queries(first, slot):
        for half in range(2):
            parts = []
            for a in range(2):
                b = order[first + 2 * half + a]
                four = q_ref[b // 4].astype(F32)
                two = jnp.where(b % 4 >= 2, four[:, 128:], four[:, :128])
                parts.append(jnp.where(b % 2 == a, two, pltpu.roll(two, 64, 1)))
            q = jnp.where(lane < 64, *parts)
            qt[slot, :64, 128 * half : 128 * half + 128] = q.astype(BF16)
        qt[slot, 64:] = jnp.zeros((64, 256), BF16)

    def raw_scores(i, slot):
        return [dot(keys, qt[slot], 1, 0) for keys in keys_of(i)]

    def keep(raw, limit, store):
        peaks = []
        for part, scores in enumerate(raw):
            rows = pl.ds(256 * part, 256)
            scores = scores * SCALE_LOG2
            if limit is not None:
                scores = jnp.where(gap[rows] <= limit, scores, NEG)
            store[rows] = scores
            peaks.append(jnp.max(scores, axis=0, keepdims=True))
        return jnp.maximum(*peaks)

    def weigh(i, store, m, acc):
        for part in range(2):
            w = jnp.exp2(store[256 * part : 256 * part + 256] - m).astype(BF16)
            acc = acc + dot(vt[i, part], w, 1, 0)
        return acc

    def step(i, states):
        raw = [raw_scores(i + 1, slot) for slot in range(2)]
        done = []
        for slot in range(2):
            m, acc, peak = states[slot]
            new = jnp.maximum(m, peak)
            acc = weigh(i, s.at[slot], new, acc * jnp.exp2(m - new))
            done.append((new, acc, keep(raw[slot], None, s.at[slot])))
        return tuple(done)

    def finish(first, acc):
        out = acc[:64] / acc[64:65]
        out = jnp.concatenate([out, jnp.zeros((64, 256), F32)], axis=0).T
        for a in range(4):
            top, low = out[64 * a : 64 * a + 32], out[64 * a + 32 : 64 * a + 64]
            o_ref[first + a] = (top + pltpu.roll(low, 64, 1)).astype(BF16)

    def tiles(j, _):
        base = 8 * j
        for slot in range(2):
            load_queries(base + 4 * slot, slot)
        def turn(i):
            for part, keys in enumerate(keys_of(i)):
                vt[i, part, :64] = keys.T[64:]

        def three(u):
            first = jnp.where(u == 4, 0, base + u)
            last = jnp.where(u == 4, 0, base + 4 + u)
            limit = jnp.where(u == 4, 32 * BLK, -u * BLK)
            raw = raw_scores(first, 0), raw_scores(first, 1), raw_scores(last, 1)
            return raw, (limit, None, limit)

        def keep_three(raw, limits):
            return tuple(keep(raw[n], limits[n], s.at[n]) for n in range(3))

        def near(u, carry):
            (m0, acc0), (m1, acc1), (p0, p1, p2) = carry
            raw, limits = three(u + 1)
            turn(base + u)
            turn(base + 4 + u)
            n0 = jnp.maximum(m0, p0)
            n1 = jnp.maximum(m1, jnp.maximum(p1, p2))
            acc0 = weigh(base + u, s.at[0], n0, acc0 * jnp.exp2(m0 - n0))
            acc1 = weigh(base + u, s.at[1], n1, acc1 * jnp.exp2(m1 - n1))
            acc1 = weigh(base + 4 + u, s.at[2], n1, acc1)
            return (n0, acc0), (n1, acc1), keep_three(raw, limits)

        m = jnp.full((1, 256), sink, F32)
        carry = (m, zero), (m, zero), keep_three(*three(0))
        carry = lax.fori_loop(0, 2, lambda t, v: near(2 * t + 1, near(2 * t, v)), carry)
        states = tuple((*carry[slot], carry[2][slot]) for slot in range(2))

        def four(t, states):
            for n in range(4):
                states = step(4 * t + n, states)
            return states

        states = lax.fori_loop(0, 2 * j, four, states)
        for slot in range(2):
            finish(base + 4 * slot, states[slot][1])
        return 0

    lax.fori_loop(0, NBLK // 8, tiles, 0)


def return_part(places, o_ref, out, held, own, send, recv):
    z, y, x, c = place()
    for b in range(NBLK):
        own[b] = o_ref[places[b]]
    held[z * 4 + y] = own[z * 4 + y]

    def copy(k, block, head, target):
        return pltpu.make_async_remote_copy(
            src_ref=own.at[block],
            dst_ref=held.at[head],
            send_sem=send.at[k],
            recv_sem=recv.at[k],
            device_id=target,
            device_id_type=MESH,
        )

    def sent(k):
        dz, dy = OFFSETS[k]
        zz, yy = (z + dz) % 8, (y + dy) % 4
        return copy(k, zz * 4 + yy, z * 4 + y, dev(zz, yy, x, c))

    for k in range(31):
        sent(k).start()
    for k, (dz, dy) in enumerate(OFFSETS):
        zz, yy = (z + 8 - dz) % 8, (y + 4 - dy) % 4
        copy(k, 0, zz * 4 + yy, dev(zz, yy, x, c)).wait_recv()
    lane = lax.broadcasted_iota(I32, (32, 128), 1)
    for k in range(16):
        p, q = held[2 * k].astype(F32), held[2 * k + 1].astype(F32)
        cols = pl.ds(128 * k, 128)
        out[:32, cols] = jnp.where(lane < 64, p, pltpu.roll(q, 64, 1)).astype(BF16)
        out[32:, cols] = jnp.where(lane < 64, pltpu.roll(p, 64, 1), q).astype(BF16)
    for k in range(31):
        sent(k).wait_send()


def kernel(
    places, sinks, inv_row, inv_col, tok_hbm, wqt_hbm, kvw_hbm, out,
    q, kv, order, tok, wts, kvw, kvp, stage, mid, angles,
    lsem, send, recv, zsend, zrecv, psend, precv, ysend, yrecv, qsend, qrecv, known,
    attended, vt, qt, gap, s, held, own, osend, orecv,
):
    prepare_part(
        places, inv_row, inv_col, tok_hbm, wqt_hbm, kvw_hbm, q, kv, order,
        tok, wts, kvw, kvp, stage, mid, angles,
        lsem, send, recv, zsend, zrecv, psend, precv, ysend, yrecv, qsend, qrecv, known,
    )
    attend_part(sinks, q, kv, attended, order, vt, qt, gap, s)
    return_part(places, attended, out, held, own, osend, orecv)


def per_device(tokens, query_weight, key_value_weight, block_places, sinks):
    dma = pltpu.SemaphoreType.DMA
    return pl.pallas_call(
        kernel,
        in_specs=[SMEM, SMEM, VMEM, VMEM, HBM, HBM, HBM],
        out_specs=VMEM,
        out_shape=jax.ShapeDtypeStruct((64, 2048), BF16),
        scratch_shapes=[
            pltpu.VMEM((8, 64, 256), BF16),
            pltpu.VMEM((2, 4, 4, 8, 64, 128), BF16),
            pltpu.SMEM((NBLK,), I32),
            pltpu.VMEM((4, 2, 32, WIDTH), BF16),
            pltpu.VMEM((4, 2, 2, 32, WIDTH), BF16),
            pltpu.VMEM((WIDTH, 1024), BF16),
            pltpu.VMEM((8, 64, 128), BF16),
            pltpu.VMEM((4, 2, 64, 256), BF16),
            pltpu.VMEM((8, 64, 256), BF16),
            pltpu.VMEM((2, 32, 256), F32),
            dma((6,)),
            dma((42,)),
            dma((42,)),
            dma((7,)),
            dma((7,)),
            dma((20,)),
            dma((20,)),
            dma((8,)),
            dma((8,)),
            dma((8,)),
            dma((8,)),
            pltpu.SemaphoreType.REGULAR((4,)),
            pltpu.VMEM((NBLK, 32, 128), BF16),
            pltpu.VMEM((NBLK, 2, 80, 256), BF16),
            pltpu.VMEM((2, 128, 256), BF16),
            pltpu.VMEM((BLK, 256), I32),
            pltpu.VMEM((3, BLK, 256), F32),
            pltpu.VMEM((NBLK, 32, 128), BF16),
            pltpu.VMEM((NBLK, 32, 128), BF16),
            dma((31,)),
            dma((31,)),
        ],
        compiler_params=pltpu.CompilerParams(collective_id=1, has_side_effects=True),
        name="layer",
    )(
        block_places,
        sinks,
        jnp.asarray(np.tile(INVERSE, 4)[None, :]),
        jnp.asarray(np.tile(INVERSE[:, None], (1, 128))),
        tokens.reshape(2, 32, WIDTH),
        query_weight.T.reshape(2, 32, WIDTH),
        key_value_weight,
    )


def solution(mesh):
    in_specs = (P(("grp", "sp"), None), P(None, "sp"), P(), P(), P())
    return jax.shard_map(
        per_device,
        mesh=mesh,
        in_specs=in_specs,
        out_specs=P(("grp", "sp"), None),
        check_vma=False,
    )
```

```python
import math

import jax
import jax.numpy as jnp
import numpy as np
from jax import lax
from jax.experimental import pallas as pl
from jax.experimental.pallas import tpu as pltpu
from jax.sharding import PartitionSpec as P

MESH = pl.DeviceIdType.MESH
BF16, F32, I32 = jnp.bfloat16, jnp.float32, jnp.int32
WIDTH = 2880
HEAD = 64
BLK = 512
NBLK = 32
SCALE_LOG2 = HEAD**-0.5 * math.log2(math.e)
NEG = -1e30
VMEM = pl.BlockSpec(memory_space=pltpu.VMEM)
HBM = pl.BlockSpec(memory_space=pltpu.HBM)
SMEM = pl.BlockSpec(memory_space=pltpu.SMEM)
OFFSETS = [(dz, dy) for dz in range(8) for dy in range(4) if dz or dy]
OFFSETS.sort(key=lambda o: -(min(o[0], 8 - o[0]) + min(o[1], 4 - o[1])))
INVERSE = (150000.0 ** (-(np.arange(32, dtype=np.float64) * 2.0) / HEAD)).astype(np.float32)


def place():
    z = lax.axis_index("grp")
    s = lax.axis_index("sp")
    return z, s // 8, (s // 2) % 4, s % 2


def dev(z, y, x, c):
    return (z, (y * 4 + x) * 2 + c)


def dot(a, b, ca, cb):
    return lax.dot_general(a, b, (((ca,), (cb,)), ((), ())), preferred_element_type=F32)


class Ring:
    def __init__(self, at, me, right, left, send, recv, first):
        self.at, self.me, self.right, self.left = at, me, right, left
        self.send, self.recv, self.first = send, recv, first
        self.prev, self.next, self.opp = (me + 3) % 4, (me + 1) % 4, (me + 2) % 4

    def copy(self, piece, half, target, k):
        ref = self.at(piece, half)
        return pltpu.make_async_remote_copy(
            src_ref=ref,
            dst_ref=ref,
            send_sem=self.send.at[self.first + k],
            recv_sem=self.recv.at[self.first + k],
            device_id=target,
            device_id_type=MESH,
        )

    def start(self):
        self.copy(self.me, 0, self.right, 0).start()
        self.copy(self.me, 1, self.left, 2).start()
        self.copy(self.me, 1, self.right, 1).start()
        self.copy(self.me, 0, self.left, 3).start()

    def forward(self):
        self.copy(self.prev, 0, self.right, 0).wait_recv()
        self.copy(self.prev, 0, self.right, 4).start()
        self.copy(self.next, 1, self.left, 2).wait_recv()
        self.copy(self.next, 1, self.left, 5).start()

    def near(self):
        self.copy(self.prev, 1, self.right, 1).wait_recv()
        self.copy(self.next, 0, self.left, 3).wait_recv()

    def far(self):
        self.copy(self.opp, 0, self.right, 4).wait_recv()
        self.copy(self.opp, 1, self.left, 5).wait_recv()

    def drain(self):
        self.copy(self.me, 0, self.right, 0).wait_send()
        self.copy(self.me, 1, self.right, 1).wait_send()
        self.copy(self.me, 1, self.left, 2).wait_send()
        self.copy(self.me, 0, self.left, 3).wait_send()
        self.copy(self.prev, 0, self.right, 4).wait_send()
        self.copy(self.next, 1, self.left, 5).wait_send()


def prepare_part(
    idle, queries_here, small, places, inv_row, inv_col, tok_hbm, wqt_hbm, kvw_hbm, q_out, kv, order,
    tok, wts, kvw, kvp, stage, mid, angles, lsem, send, recv, zsend, zrecv, psend, precv, ysend, yrecv, qsend, qrecv, known,
):
    z, y, x, c = place()
    o = 1 - c
    a, b = x * o + y * c, y * o + x * c
    partner = dev(z, y, x, o)
    ring_y = (dev(z, (y + 1) % 4, x, c), dev(z, (y + 3) % 4, x, c))
    ring_x = (dev(z, y, (x + 1) % 4, c), dev(z, y, (x + 3) % 4, c))
    others = [dev((z + d) % 8, y, x, c) for d in range(1, 8)]
    ring_z = (others[0], others[6])
    peers = [*ring_y, *ring_x, *ring_z, partner]

    def tell(targets, k):
        for target in targets:
            pl.semaphore_signal(known.at[k], inc=1, device_id=target, device_id_type=MESH)

    def hear(targets, k):
        pl.semaphore_wait(known.at[k], len(targets))

    ready = pltpu.get_barrier_semaphore()
    for peer in peers:
        pl.semaphore_signal(ready, inc=1, device_id=peer, device_id_type=MESH)

    own = [
        pltpu.make_async_copy(tok_hbm, tok.at[y], lsem.at[0]),
        pltpu.make_async_copy(wqt_hbm, wts.at[x, c], lsem.at[1]),
    ]
    for n in range(4):
        cols = pl.ds(256 * n, 256)
        own.append(pltpu.make_async_copy(kvw_hbm.at[:, cols], kvw.at[:, cols], lsem.at[2 + n]))
    for n in (0, 1):
        own[n].start()
    for copy in small:
        copy.start()
    for n in (2, 4, 3, 5):
        own[n].start()

    for copy in small:
        copy.wait()
    lane = lax.broadcasted_iota(I32, (64, 128), 1)
    base = places[z * 4 + y] * BLK + (x * 2 + c) * 64
    angle = (base + lax.broadcasted_iota(I32, (64, 128), 0)).astype(F32) * inv_row[...]
    cosine = jnp.cos(angle)
    sine = jnp.where(lane % 64 < 32, -1.0, 1.0) * jnp.sin(angle)
    own[0].wait()
    own[1].wait()
    pl.semaphore_wait(ready, len(peers))

    tok_ring = Ring(lambda p, h: tok.at[p, h], y, *ring_y, send, recv, 0)
    wts_ring = Ring(lambda p, h: wts.at[p, c, h], x, *ring_x, send, recv, 6)
    near = [
        dev(z, (y + c) % 4, (x + o) % 4, c),
        dev(z, (y + 3 * c) % 4, (x + 3 * o) % 4, c),
    ]
    wide = [
        dev(z, (y + o) % 4, (x + c) % 4, c),
        dev(z, (y + 3 * o) % 4, (x + 3 * c) % 4, c),
    ]
    kv1_ring = Ring(lambda p, h: kv.at[c, b, p, pl.ds(4 * h, 4)], a, *near, send, recv, 12)
    kv2_rings = [
        Ring(
            lambda p, h, piece=(a + d) % 4: kv.at[c, p, piece, pl.ds(4 * h, 4)],
            b, *wide, send, recv, 18 + 6 * d,
        )
        for d in range(4)
    ]

    def with_partner(ref, k):
        return pltpu.make_async_remote_copy(
            src_ref=ref,
            dst_ref=ref,
            send_sem=psend.at[k],
            recv_sem=precv.at[k],
            device_id=partner,
            device_id_type=MESH,
        )

    def piece(n, p):
        return with_partner(kv.at[c, (b + n) % 4, (a + p) % 4], 4 + 4 * n + p)

    def exchange(d, head, source):
        return pltpu.make_async_remote_copy(
            src_ref=kvp.at[head],
            dst_ref=kv.at[c, b, a, source],
            send_sem=zsend.at[d - 1],
            recv_sem=zrecv.at[d - 1],
            device_id=others[d - 1],
            device_id_type=MESH,
        )

    tok_ring.start()
    wts_ring.start()
    with_partner(wts.at[x, c], 0).start()
    tell(ring_z, 0)
    tell(ring_y, 1)

    rows = tok[y].reshape(64, WIDTH)
    for n in range(2):
        own[2 + n].wait()
        own[4 + n].wait()
        keys = jnp.dot(rows, kvw[:, 256 * n : 256 * n + 256], preferred_element_type=F32)
        values = jnp.dot(rows, kvw[:, 512 + 256 * n : 768 + 256 * n], preferred_element_type=F32)
        for p in range(2):
            k, v = keys[:, 128 * p : 128 * p + 128], values[:, 128 * p : 128 * p + 128]
            swapped = jnp.where(lane % 64 < 32, pltpu.roll(k, 96, 1), pltpu.roll(k, 32, 1))
            k = k * cosine + swapped * sine
            kvp[4 * n + 2 * p] = jnp.where(lane < 64, k, pltpu.roll(v, 64, 1)).astype(BF16)
            kvp[4 * n + 2 * p + 1] = jnp.where(lane < 64, pltpu.roll(k, 64, 1), v).astype(BF16)
    kv[c, b, a, z] = kvp[z]
    hear(ring_z, 0)
    far_z = (others[1], others[5])
    tell(far_z, 2)
    hear(ring_y, 1)
    hear(far_z, 2)
    all_y = [dev(z, (y + d) % 4, x, c) for d in (1, 2, 3)]
    tell(all_y, 3)

    for d in (4, 3, 5, 2, 6, 1, 7):
        exchange(d, (z + d) % 8, z).start()

    col = lax.broadcasted_iota(I32, (32, 256), 1)
    block = jnp.where(
        col < 128,
        jnp.where(col < 64, places[z * 4], places[z * 4 + 1]),
        jnp.where(col < 192, places[z * 4 + 2], places[z * 4 + 3]),
    )
    angle = (block * BLK + (x * 2 + c) * 64 + col % 64).astype(F32)
    angle = angle * jnp.concatenate([inv_col[...], inv_col[...]], axis=1)
    angles[0], angles[1] = jnp.cos(angle), jnp.sin(angle)
    def place_block(i, _):
        found = 0
        for n in range(NBLK):
            found = jnp.where(places[n] == i, n, found)
        order[i] = found
        return 0

    lax.fori_loop(0, NBLK, place_block, 0)
    idle()
    for d in range(1, 8):
        exchange(d, z, (z + 8 - d) % 8).wait_recv()
    kv1_ring.start()
    kv2_rings[0].start()
    wts_ring.forward()
    tok_ring.forward()
    wts_ring.near()
    with_partner(wts.at[(x + 3) % 4, c], 1).start()
    with_partner(wts.at[(x + 1) % 4, c], 2).start()
    tok_ring.near()
    kv1_ring.forward()
    kv2_rings[0].forward()
    kv1_ring.near()
    kv2_rings[1].start()
    kv2_rings[3].start()
    wts_ring.far()
    with_partner(wts.at[(x + 2) % 4, c], 3).start()
    tok_ring.far()
    with_partner(wts.at[x, o], 0).wait_recv()
    with_partner(wts.at[(x + 3) % 4, o], 1).wait_recv()
    with_partner(wts.at[(x + 1) % 4, o], 2).wait_recv()
    with_partner(wts.at[(x + 2) % 4, o], 3).wait_recv()

    hear(all_y, 3)
    def along_y(d, half, target, source):
        return pltpu.make_async_remote_copy(
            src_ref=stage.at[target, half],
            dst_ref=mid.at[2 * source + half],
            send_sem=ysend.at[2 * d + half],
            recv_sem=yrecv.at[2 * d + half],
            device_id=dev(z, (y + d) % 4, x, c),
            device_id_type=MESH,
        )

    def along_z(d, half):
        plane = 2 * ((y + 4 - d) % 4) + half
        return plane, pltpu.make_async_remote_copy(
            src_ref=mid.at[plane],
            dst_ref=q_out.at[z],
            send_sem=qsend.at[2 * d + half],
            recv_sem=qrecv.at[z],
            device_id=dev(plane, y, x, c),
            device_id_type=MESH,
        )

    def pass_on(d, half):
        plane, copy = along_z(d, half)

        @pl.when(plane != z)
        def _():
            copy.start()

        @pl.when(plane == z)
        def _():
            q_out[z] = mid[plane]

    rows = tok[...].reshape(256, WIDTH)
    for half in range(2):
        w = wts[2 * half : 2 * half + 2].reshape(256, WIDTH)
        q = dot(w, rows, 1, 1)
        for i in range(4):
            lo, hi = q[i * 64 : i * 64 + 32], q[i * 64 + 32 : i * 64 + 64]
            stage[i, half, :32] = (lo * angles[0] - hi * angles[1]).astype(BF16)
            stage[i, half, 32:] = (hi * angles[0] + lo * angles[1]).astype(BF16)
        for d in (2, 1, 3):
            along_y(d, half, (y + d) % 4, y).start()
        mid[2 * y + half] = stage[y, half]
    for half in range(2):
        pass_on(0, half)

    kv1_ring.far()
    kv2_rings[2].start()
    for p in range(4):
        piece(0, p).start()
    kv2_rings[1].forward()
    kv2_rings[3].forward()

    for half in range(2):
        for d in (1, 3, 2):
            along_y(d, half, y, (y + 4 - d) % 4).wait_recv()
            pass_on(d, half)

    kv2_rings[2].forward()
    for p in (0, 1, 3, 2):
        kv2_rings[p].near()
        piece(1, p).start()
        piece(3, p).start()
    for p in (0, 1, 3, 2):
        kv2_rings[p].far()
        piece(2, p).start()

    for g in range(8):

        @pl.when(g != z)
        def _():
            pltpu.make_async_remote_copy(
                src_ref=mid.at[0],
                dst_ref=q_out.at[g],
                send_sem=qsend.at[0],
                recv_sem=qrecv.at[g],
                device_id=dev(g, y, x, c),
                device_id_type=MESH,
            ).wait_recv()

    queries_here()
    for n in range(4):
        for p in range(4):
            with_partner(kv.at[o, (a + n) % 4, (b + p) % 4], 4 + 4 * n + p).wait_recv()
    for ring in (tok_ring, wts_ring, kv1_ring, *kv2_rings):
        ring.drain()
    for d in range(1, 8):
        exchange(d, (z + d) % 8, z).wait_send()
    for half in range(2):
        for d in range(1, 4):
            along_y(d, half, (y + d) % 4, y).wait_send()
        for d in range(4):
            plane, copy = along_z(d, half)

            @pl.when(plane != z)
            def _():
                copy.wait_send()

    with_partner(wts.at[x, c], 0).wait_send()
    with_partner(wts.at[(x + 3) % 4, c], 1).wait_send()
    with_partner(wts.at[(x + 1) % 4, c], 2).wait_send()
    with_partner(wts.at[(x + 2) % 4, c], 3).wait_send()
    for n in range(4):
        for p in range(4):
            piece(n, p).wait_send()


def attend_tables(vt, gap):
    z, y, x, c = place()
    offset = (x * 2 + c) * 64
    key = lax.broadcasted_iota(I32, (BLK, 256), 0)
    col = lax.broadcasted_iota(I32, (BLK, 256), 1)
    key = ((key >> 6) & 3) * 128 + (key >> 8) * 64 + (key & 63)
    gap[...] = key - ((col >> 6) * BLK + offset + (col & 63))
    vt[...] = jnp.ones((NBLK, 2, 80, 256), BF16)


def attend_queries(q_ref, order, qt):
    lane = lax.broadcasted_iota(I32, (64, 128), 1)

    def load_queries(tile, _):
        for half in range(2):
            parts = []
            for a in range(2):
                b = order[4 * tile + 2 * half + a]
                four = q_ref[b // 4].astype(F32)
                two = jnp.where(b % 4 >= 2, four[:, 128:], four[:, :128])
                parts.append(jnp.where(b % 2 == a, two, pltpu.roll(two, 64, 1)))
            q = jnp.where(lane < 64, *parts)
            qt[tile, :64, 128 * half : 128 * half + 128] = q.astype(BF16)
        qt[tile, 64:] = jnp.zeros((64, 256), BF16)
        return 0

    lax.fori_loop(0, 8, load_queries, 0, unroll=4)


def attend_part(sinks, kv_ref, o_ref, order, vt, qt, gap, s):
    z, y, x, c = place()
    sink = sinks[z * 4 + y] * math.log2(math.e)

    def keys_of(i):
        b = order[i]
        g, r = b // 4, b % 4
        return kv_ref[0, r, :, g].reshape(256, 128), kv_ref[1, :, r, g].reshape(256, 128)

    zero = jnp.where(lax.broadcasted_iota(I32, (80, 256), 0) < 64, 0.0, 1.0)

    def raw_scores(i, tile):
        return [dot(keys, qt[tile], 1, 0) for keys in keys_of(i)]

    def keep(raw, limit, store):
        peaks = []
        for part, scores in enumerate(raw):
            rows = pl.ds(256 * part, 256)
            scores = scores * SCALE_LOG2
            if limit is not None:
                scores = jnp.where(gap[rows] <= limit, scores, NEG)
            store[rows] = scores
            peaks.append(jnp.max(scores, axis=0, keepdims=True))
        return jnp.maximum(*peaks)

    def weigh(i, store, m, acc):
        for part in range(2):
            w = jnp.exp2(store[256 * part : 256 * part + 256] - m).astype(BF16)
            acc = acc + dot(vt[i, part], w, 1, 0)
        return acc

    def finish(first, acc):
        out = acc[:64] / acc[64:65]
        out = jnp.concatenate([out, jnp.zeros((64, 256), F32)], axis=0).T
        for a in range(4):
            top, low = out[64 * a : 64 * a + 32], out[64 * a + 32 : 64 * a + 64]
            o_ref[first + a] = (top + pltpu.roll(low, 64, 1)).astype(BF16)

    def turn(i):
        for part, keys in enumerate(keys_of(i)):
            vt[i, part, :64] = keys.T[64:]

    def three(j, u):
        raw = (
            raw_scores(8 * j + u, 2 * j),
            raw_scores(8 * j + u, 2 * j + 1),
            raw_scores(8 * j + 4 + u, 2 * j + 1),
        )
        return raw, (-u * BLK, None, -u * BLK)

    def keep_three(raw, limits):
        return tuple(keep(raw[n], limits[n], s.at[n]) for n in range(3))

    def tiles(j, peaks):
        base = 8 * j

        def step(i, states):
            raw = [raw_scores(i + 1, 2 * j + slot) for slot in range(2)]
            done = []
            for slot in range(2):
                m, acc, peak = states[slot]
                new = jnp.maximum(m, peak)
                acc = weigh(i, s.at[slot], new, acc * jnp.exp2(m - new))
                done.append((new, acc, keep(raw[slot], None, s.at[slot])))
            return tuple(done)

        m = jnp.full((1, 256), sink, F32)
        carry = (m, zero), (m, zero), peaks
        for u in range(4):
            (m0, acc0), (m1, acc1), (p0, p1, p2) = carry
            if u < 3:
                raw, limits = three(j, u + 1)
            else:
                raw = [raw_scores(0, 2 * j), raw_scores(0, 2 * j + 1)]
            turn(base + u)
            turn(base + 4 + u)
            n0 = jnp.maximum(m0, p0)
            n1 = jnp.maximum(m1, jnp.maximum(p1, p2))
            acc0 = weigh(base + u, s.at[0], n0, acc0 * jnp.exp2(m0 - n0))
            acc1 = weigh(base + u, s.at[1], n1, acc1 * jnp.exp2(m1 - n1))
            acc1 = weigh(base + 4 + u, s.at[2], n1, acc1)
            if u < 3:
                peaks = keep_three(raw, limits)
            else:
                peaks = [keep(raw[n], None, s.at[n]) for n in range(2)]
            carry = (n0, acc0), (n1, acc1), peaks
        states = tuple((*carry[slot], carry[2][slot]) for slot in range(2))

        def eight(t, states):
            for n in range(8):
                states = step(8 * t + n, states)
            return states

        states = lax.fori_loop(0, j, eight, states)
        peaks = keep_three(*three(jnp.minimum(j + 1, 3), 0))
        for slot in range(2):
            finish(base + 4 * slot, states[slot][1])
        return peaks

    lax.fori_loop(0, NBLK // 8, tiles, keep_three(*three(0, 0)))


def return_part(places, o_ref, out, held, own, send, recv):
    z, y, x, c = place()
    for b in range(NBLK):
        own[b] = o_ref[places[b]]
    held[z * 4 + y] = own[z * 4 + y]

    def copy(k, block, head, target):
        return pltpu.make_async_remote_copy(
            src_ref=own.at[block],
            dst_ref=held.at[head],
            send_sem=send.at[k],
            recv_sem=recv.at[k],
            device_id=target,
            device_id_type=MESH,
        )

    def sent(k):
        dz, dy = OFFSETS[k]
        zz, yy = (z + dz) % 8, (y + dy) % 4
        return copy(k, zz * 4 + yy, z * 4 + y, dev(zz, yy, x, c))

    for k in range(31):
        sent(k).start()
    for k, (dz, dy) in enumerate(OFFSETS):
        zz, yy = (z + 8 - dz) % 8, (y + 4 - dy) % 4
        copy(k, 0, zz * 4 + yy, dev(zz, yy, x, c)).wait_recv()
    lane = lax.broadcasted_iota(I32, (32, 128), 1)
    for k in range(16):
        p, q = held[2 * k].astype(F32), held[2 * k + 1].astype(F32)
        cols = pl.ds(128 * k, 128)
        out[:32, cols] = jnp.where(lane < 64, p, pltpu.roll(q, 64, 1)).astype(BF16)
        out[32:, cols] = jnp.where(lane < 64, pltpu.roll(p, 64, 1), q).astype(BF16)
    for k in range(31):
        sent(k).wait_send()


def kernel(
    places_hbm, sinks_hbm, row_hbm, col_hbm, tok_hbm, wqt_hbm, kvw_hbm, out,
    places, sinks, inv_row, inv_col, ssem,
    q, kv, order, tok, wts, kvw, kvp, stage, mid, angles,
    lsem, send, recv, zsend, zrecv, psend, precv, ysend, yrecv, qsend, qrecv, known,
    attended, vt, qt, gap, s, held, own, osend, orecv,
):
    small = [
        pltpu.make_async_copy(places_hbm, places, ssem.at[0]),
        pltpu.make_async_copy(sinks_hbm, sinks, ssem.at[1]),
        pltpu.make_async_copy(row_hbm, inv_row, ssem.at[2]),
        pltpu.make_async_copy(col_hbm, inv_col, ssem.at[3]),
    ]
    prepare_part(
        lambda: attend_tables(vt, gap), lambda: attend_queries(q, order, qt),
        small, places, inv_row, inv_col, tok_hbm, wqt_hbm, kvw_hbm, q, kv, order,
        tok, wts, kvw, kvp, stage, mid, angles,
        lsem, send, recv, zsend, zrecv, psend, precv, ysend, yrecv, qsend, qrecv, known,
    )
    attend_part(sinks, kv, attended, order, vt, qt, gap, s)
    return_part(places, attended, out, held, own, osend, orecv)


def per_device(tokens, query_weight, key_value_weight, block_places, sinks):
    dma = pltpu.SemaphoreType.DMA
    return pl.pallas_call(
        kernel,
        in_specs=[HBM] * 7,
        out_specs=VMEM,
        out_shape=jax.ShapeDtypeStruct((64, 2048), BF16),
        scratch_shapes=[
            pltpu.SMEM((NBLK,), I32),
            pltpu.SMEM((32,), F32),
            pltpu.VMEM((1, 128), F32),
            pltpu.VMEM((32, 128), F32),
            dma((4,)),
            pltpu.VMEM((8, 64, 256), BF16),
            pltpu.VMEM((2, 4, 4, 8, 64, 128), BF16),
            pltpu.SMEM((NBLK,), I32),
            pltpu.VMEM((4, 2, 32, WIDTH), BF16),
            pltpu.VMEM((4, 2, 2, 32, WIDTH), BF16),
            pltpu.VMEM((WIDTH, 1024), BF16),
            pltpu.VMEM((8, 64, 128), BF16),
            pltpu.VMEM((4, 2, 64, 256), BF16),
            pltpu.VMEM((8, 64, 256), BF16),
            pltpu.VMEM((2, 32, 256), F32),
            dma((6,)),
            dma((42,)),
            dma((42,)),
            dma((7,)),
            dma((7,)),
            dma((20,)),
            dma((20,)),
            dma((8,)),
            dma((8,)),
            dma((8,)),
            dma((8,)),
            pltpu.SemaphoreType.REGULAR((4,)),
            pltpu.VMEM((NBLK, 32, 128), BF16),
            pltpu.VMEM((NBLK, 2, 80, 256), BF16),
            pltpu.VMEM((8, 128, 256), BF16),
            pltpu.VMEM((BLK, 256), I32),
            pltpu.VMEM((3, BLK, 256), F32),
            pltpu.VMEM((NBLK, 32, 128), BF16),
            pltpu.VMEM((NBLK, 32, 128), BF16),
            dma((31,)),
            dma((31,)),
        ],
        compiler_params=pltpu.CompilerParams(collective_id=1, has_side_effects=True),
        name="layer",
    )(
        block_places,
        sinks,
        jnp.asarray(np.tile(INVERSE, 4)[None, :]),
        jnp.asarray(np.tile(INVERSE[:, None], (1, 128))),
        tokens.reshape(2, 32, WIDTH),
        query_weight.T.reshape(2, 32, WIDTH),
        key_value_weight,
    )


def solution(mesh):
    in_specs = (P(("grp", "sp"), None), P(None, "sp"), P(), P(), P())
    return jax.shard_map(
        per_device,
        mesh=mesh,
        in_specs=in_specs,
        out_specs=P(("grp", "sp"), None),
        check_vma=False,
    )
```

```python
import math

import jax
import jax.numpy as jnp
import numpy as np
from jax import lax
from jax.experimental import pallas as pl
from jax.experimental.pallas import tpu as pltpu
from jax.sharding import PartitionSpec as P

MESH = pl.DeviceIdType.MESH
BF16, F32, I32 = jnp.bfloat16, jnp.float32, jnp.int32
WIDTH = 2880
HEAD = 64
BLK = 512
NBLK = 32
SCALE_LOG2 = HEAD**-0.5 * math.log2(math.e)
NEG = -1e30
VMEM = pl.BlockSpec(memory_space=pltpu.VMEM)
HBM = pl.BlockSpec(memory_space=pltpu.HBM)
SMEM = pl.BlockSpec(memory_space=pltpu.SMEM)
OFFSETS = [(dz, dy) for dz in range(8) for dy in range(4) if dz or dy]
OFFSETS.sort(key=lambda o: -(min(o[0], 8 - o[0]) + min(o[1], 4 - o[1])))
INVERSE = (150000.0 ** (-(np.arange(32, dtype=np.float64) * 2.0) / HEAD)).astype(np.float32)


def place():
    z = lax.axis_index("grp")
    s = lax.axis_index("sp")
    return z, s // 8, (s // 2) % 4, s % 2


def dev(z, y, x, c):
    return (z, (y * 4 + x) * 2 + c)


def dot(a, b, ca, cb):
    return lax.dot_general(a, b, (((ca,), (cb,)), ((), ())), preferred_element_type=F32)


class Ring:
    def __init__(self, at, me, right, left, send, recv, first):
        self.at, self.me, self.right, self.left = at, me, right, left
        self.send, self.recv, self.first = send, recv, first
        self.prev, self.next, self.opp = (me + 3) % 4, (me + 1) % 4, (me + 2) % 4

    def copy(self, piece, half, target, k):
        ref = self.at(piece, half)
        return pltpu.make_async_remote_copy(
            src_ref=ref,
            dst_ref=ref,
            send_sem=self.send.at[self.first + k],
            recv_sem=self.recv.at[self.first + k],
            device_id=target,
            device_id_type=MESH,
        )

    def start(self):
        self.copy(self.me, 0, self.right, 0).start()
        self.copy(self.me, 1, self.left, 2).start()
        self.copy(self.me, 1, self.right, 1).start()
        self.copy(self.me, 0, self.left, 3).start()

    def forward(self):
        self.copy(self.prev, 0, self.right, 0).wait_recv()
        self.copy(self.prev, 0, self.right, 4).start()
        self.copy(self.next, 1, self.left, 2).wait_recv()
        self.copy(self.next, 1, self.left, 5).start()

    def near(self):
        self.copy(self.prev, 1, self.right, 1).wait_recv()
        self.copy(self.next, 0, self.left, 3).wait_recv()

    def far(self):
        self.copy(self.opp, 0, self.right, 4).wait_recv()
        self.copy(self.opp, 1, self.left, 5).wait_recv()

    def drain(self):
        self.copy(self.me, 0, self.right, 0).wait_send()
        self.copy(self.me, 1, self.right, 1).wait_send()
        self.copy(self.me, 1, self.left, 2).wait_send()
        self.copy(self.me, 0, self.left, 3).wait_send()
        self.copy(self.prev, 0, self.right, 4).wait_send()
        self.copy(self.next, 1, self.left, 5).wait_send()


def prepare_part(
    idle, queries_here, small, places, inv_row, inv_col, tok_hbm, wqt_hbm, kvw_hbm, q_out, kv, order,
    tok, wts, kvw, kvp, stage, mid, angles, lsem, send, recv, zsend, zrecv, psend, precv, ysend, yrecv, qsend, qrecv, known,
):
    z, y, x, c = place()
    o = 1 - c
    a, b = x * o + y * c, y * o + x * c
    partner = dev(z, y, x, o)
    ring_y = (dev(z, (y + 1) % 4, x, c), dev(z, (y + 3) % 4, x, c))
    ring_x = (dev(z, y, (x + 1) % 4, c), dev(z, y, (x + 3) % 4, c))
    others = [dev((z + d) % 8, y, x, c) for d in range(1, 8)]
    ring_z = (others[0], others[6])
    peers = [*ring_y, *ring_x, *ring_z, partner]

    def tell(targets, k):
        for target in targets:
            pl.semaphore_signal(known.at[k], inc=1, device_id=target, device_id_type=MESH)

    def hear(targets, k):
        pl.semaphore_wait(known.at[k], len(targets))

    ready = pltpu.get_barrier_semaphore()
    for peer in peers:
        pl.semaphore_signal(ready, inc=1, device_id=peer, device_id_type=MESH)

    own = [
        pltpu.make_async_copy(tok_hbm, tok.at[y], lsem.at[0]),
        pltpu.make_async_copy(wqt_hbm, wts.at[x, c], lsem.at[1]),
    ]
    for n in range(4):
        cols = pl.ds(256 * n, 256)
        own.append(pltpu.make_async_copy(kvw_hbm.at[:, cols], kvw.at[:, cols], lsem.at[2 + n]))
    for n in (0, 1):
        own[n].start()
    for copy in small:
        copy.start()
    for n in (2, 4, 3, 5):
        own[n].start()

    for copy in small:
        copy.wait()
    lane = lax.broadcasted_iota(I32, (64, 128), 1)
    base = places[z * 4 + y] * BLK + (x * 2 + c) * 64
    angle = (base + lax.broadcasted_iota(I32, (64, 128), 0)).astype(F32) * inv_row[...]
    cosine = jnp.cos(angle)
    sine = jnp.where(lane % 64 < 32, -1.0, 1.0) * jnp.sin(angle)
    own[0].wait()
    own[1].wait()
    pl.semaphore_wait(ready, len(peers))

    tok_ring = Ring(lambda p, h: tok.at[p, h], y, *ring_y, send, recv, 0)
    wts_ring = Ring(lambda p, h: wts.at[p, c, h], x, *ring_x, send, recv, 6)
    near = [
        dev(z, (y + c) % 4, (x + o) % 4, c),
        dev(z, (y + 3 * c) % 4, (x + 3 * o) % 4, c),
    ]
    wide = [
        dev(z, (y + o) % 4, (x + c) % 4, c),
        dev(z, (y + 3 * o) % 4, (x + 3 * c) % 4, c),
    ]
    kv1_ring = Ring(lambda p, h: kv.at[c, b, p, pl.ds(4 * h, 4)], a, *near, send, recv, 12)
    kv2_rings = [
        Ring(
            lambda p, h, piece=(a + d) % 4: kv.at[c, p, piece, pl.ds(4 * h, 4)],
            b, *wide, send, recv, 18 + 6 * d,
        )
        for d in range(4)
    ]

    def with_partner(ref, k):
        return pltpu.make_async_remote_copy(
            src_ref=ref,
            dst_ref=ref,
            send_sem=psend.at[k],
            recv_sem=precv.at[k],
            device_id=partner,
            device_id_type=MESH,
        )

    def piece(n, p):
        return with_partner(kv.at[c, (b + n) % 4, (a + p) % 4], 4 + 4 * n + p)

    def exchange(d, head, source):
        return pltpu.make_async_remote_copy(
            src_ref=kvp.at[head],
            dst_ref=kv.at[c, b, a, source],
            send_sem=zsend.at[d - 1],
            recv_sem=zrecv.at[d - 1],
            device_id=others[d - 1],
            device_id_type=MESH,
        )

    tok_ring.start()
    wts_ring.start()
    with_partner(wts.at[x, c], 0).start()
    tell(ring_z, 0)
    tell(ring_y, 1)

    rows = tok[y].reshape(64, WIDTH)
    for n in range(2):
        own[2 + n].wait()
        own[4 + n].wait()
        keys = jnp.dot(rows, kvw[:, 256 * n : 256 * n + 256], preferred_element_type=F32)
        values = jnp.dot(rows, kvw[:, 512 + 256 * n : 768 + 256 * n], preferred_element_type=F32)
        for p in range(2):
            k, v = keys[:, 128 * p : 128 * p + 128], values[:, 128 * p : 128 * p + 128]
            swapped = jnp.where(lane % 64 < 32, pltpu.roll(k, 96, 1), pltpu.roll(k, 32, 1))
            k = k * cosine + swapped * sine
            kvp[4 * n + 2 * p] = jnp.where(lane < 64, k, pltpu.roll(v, 64, 1)).astype(BF16)
            kvp[4 * n + 2 * p + 1] = jnp.where(lane < 64, pltpu.roll(k, 64, 1), v).astype(BF16)
    kv[c, b, a, z] = kvp[z]
    hear(ring_z, 0)
    far_z = (others[1], others[5])
    tell(far_z, 2)
    hear(ring_y, 1)
    hear(far_z, 2)
    all_y = [dev(z, (y + d) % 4, x, c) for d in (1, 2, 3)]
    tell(all_y, 3)

    for d in (4, 3, 5, 2, 6, 1, 7):
        exchange(d, (z + d) % 8, z).start()

    for d in range(1, 8):
        exchange(d, z, (z + 8 - d) % 8).wait_recv()
    kv1_ring.start()
    kv2_rings[0].start()
    col = lax.broadcasted_iota(I32, (32, 256), 1)
    block = jnp.where(
        col < 128,
        jnp.where(col < 64, places[z * 4], places[z * 4 + 1]),
        jnp.where(col < 192, places[z * 4 + 2], places[z * 4 + 3]),
    )
    angle = (block * BLK + (x * 2 + c) * 64 + col % 64).astype(F32)
    angle = angle * jnp.concatenate([inv_col[...], inv_col[...]], axis=1)
    angles[0], angles[1] = jnp.cos(angle), jnp.sin(angle)
    wts_ring.forward()
    tok_ring.forward()
    wts_ring.near()
    with_partner(wts.at[(x + 3) % 4, c], 1).start()
    with_partner(wts.at[(x + 1) % 4, c], 2).start()
    tok_ring.near()
    kv1_ring.forward()
    kv2_rings[0].forward()
    kv1_ring.near()
    kv2_rings[1].start()
    kv2_rings[3].start()
    wts_ring.far()
    with_partner(wts.at[(x + 2) % 4, c], 3).start()
    tok_ring.far()
    with_partner(wts.at[x, o], 0).wait_recv()
    with_partner(wts.at[(x + 3) % 4, o], 1).wait_recv()
    with_partner(wts.at[(x + 1) % 4, o], 2).wait_recv()
    with_partner(wts.at[(x + 2) % 4, o], 3).wait_recv()

    hear(all_y, 3)
    def along_y(d, half, target, source):
        return pltpu.make_async_remote_copy(
            src_ref=stage.at[target, half],
            dst_ref=mid.at[2 * source + half],
            send_sem=ysend.at[2 * d + half],
            recv_sem=yrecv.at[2 * d + half],
            device_id=dev(z, (y + d) % 4, x, c),
            device_id_type=MESH,
        )

    def along_z(d, half):
        plane = 2 * ((y + 4 - d) % 4) + half
        return plane, pltpu.make_async_remote_copy(
            src_ref=mid.at[plane],
            dst_ref=q_out.at[z],
            send_sem=qsend.at[2 * d + half],
            recv_sem=qrecv.at[z],
            device_id=dev(plane, y, x, c),
            device_id_type=MESH,
        )

    def pass_on(d, half):
        plane, copy = along_z(d, half)

        @pl.when(plane != z)
        def _():
            copy.start()

        @pl.when(plane == z)
        def _():
            q_out[z] = mid[plane]

    rows = tok[...].reshape(256, WIDTH)
    for half in range(2):
        w = wts[2 * half : 2 * half + 2].reshape(256, WIDTH)
        q = dot(w, rows, 1, 1)
        for i in range(4):
            lo, hi = q[i * 64 : i * 64 + 32], q[i * 64 + 32 : i * 64 + 64]
            stage[i, half, :32] = (lo * angles[0] - hi * angles[1]).astype(BF16)
            stage[i, half, 32:] = (hi * angles[0] + lo * angles[1]).astype(BF16)
        for d in (2, 1, 3):
            along_y(d, half, (y + d) % 4, y).start()
        mid[2 * y + half] = stage[y, half]
    for half in range(2):
        pass_on(0, half)

    kv1_ring.far()
    kv2_rings[2].start()
    for p in range(4):
        piece(0, p).start()
    kv2_rings[1].forward()
    kv2_rings[3].forward()

    for half in range(2):
        for d in (1, 3, 2):
            along_y(d, half, y, (y + 4 - d) % 4).wait_recv()
            pass_on(d, half)

    kv2_rings[2].forward()
    def place_block(i, _):
        found = 0
        for n in range(NBLK):
            found = jnp.where(places[n] == i, n, found)
        order[i] = found
        return 0

    lax.fori_loop(0, NBLK, place_block, 0)
    idle()
    for p in (0, 1, 3, 2):
        kv2_rings[p].near()
        piece(1, p).start()
        piece(3, p).start()
    for p in (0, 1, 3, 2):
        kv2_rings[p].far()
        piece(2, p).start()

    for g in range(8):

        @pl.when(g != z)
        def _():
            pltpu.make_async_remote_copy(
                src_ref=mid.at[0],
                dst_ref=q_out.at[g],
                send_sem=qsend.at[0],
                recv_sem=qrecv.at[g],
                device_id=dev(g, y, x, c),
                device_id_type=MESH,
            ).wait_recv()

    queries_here()
    for n in range(4):
        for p in range(4):
            with_partner(kv.at[o, (a + n) % 4, (b + p) % 4], 4 + 4 * n + p).wait_recv()
    for ring in (tok_ring, wts_ring, kv1_ring, *kv2_rings):
        ring.drain()
    for d in range(1, 8):
        exchange(d, (z + d) % 8, z).wait_send()
    for half in range(2):
        for d in range(1, 4):
            along_y(d, half, (y + d) % 4, y).wait_send()
        for d in range(4):
            plane, copy = along_z(d, half)

            @pl.when(plane != z)
            def _():
                copy.wait_send()

    with_partner(wts.at[x, c], 0).wait_send()
    with_partner(wts.at[(x + 3) % 4, c], 1).wait_send()
    with_partner(wts.at[(x + 1) % 4, c], 2).wait_send()
    with_partner(wts.at[(x + 2) % 4, c], 3).wait_send()
    for n in range(4):
        for p in range(4):
            piece(n, p).wait_send()


def attend_tables(vt, gap):
    z, y, x, c = place()
    offset = (x * 2 + c) * 64
    key = lax.broadcasted_iota(I32, (BLK, 256), 0)
    col = lax.broadcasted_iota(I32, (BLK, 256), 1)
    key = ((key >> 6) & 3) * 128 + (key >> 8) * 64 + (key & 63)
    gap[...] = key - ((col >> 6) * BLK + offset + (col & 63))
    vt[...] = jnp.ones((NBLK, 2, 80, 256), BF16)


def attend_queries(q_ref, order, qt):
    lane = lax.broadcasted_iota(I32, (64, 128), 1)

    def load_queries(tile, _):
        for half in range(2):
            parts = []
            for a in range(2):
                b = order[4 * tile + 2 * half + a]
                four = q_ref[b // 4].astype(F32)
                two = jnp.where(b % 4 >= 2, four[:, 128:], four[:, :128])
                parts.append(jnp.where(b % 2 == a, two, pltpu.roll(two, 64, 1)))
            q = jnp.where(lane < 64, *parts)
            qt[tile, :64, 128 * half : 128 * half + 128] = q.astype(BF16)
        qt[tile, 64:] = jnp.zeros((64, 256), BF16)
        return 0

    lax.fori_loop(0, 8, load_queries, 0, unroll=4)


def attend_part(sinks, kv_ref, o_ref, order, vt, qt, gap, s):
    z, y, x, c = place()
    sink = sinks[z * 4 + y] * math.log2(math.e)

    def keys_of(i):
        b = order[i]
        g, r = b // 4, b % 4
        return kv_ref[0, r, :, g].reshape(256, 128), kv_ref[1, :, r, g].reshape(256, 128)

    zero = jnp.where(lax.broadcasted_iota(I32, (80, 256), 0) < 64, 0.0, 1.0)

    def raw_scores(i, tile):
        return [dot(keys, qt[tile], 1, 0) for keys in keys_of(i)]

    def keep(raw, limit, store):
        peaks = []
        for part, scores in enumerate(raw):
            rows = pl.ds(256 * part, 256)
            scores = scores * SCALE_LOG2
            if limit is not None:
                scores = jnp.where(gap[rows] <= limit, scores, NEG)
            store[rows] = scores
            peaks.append(jnp.max(scores, axis=0, keepdims=True))
        return jnp.maximum(*peaks)

    def weigh(i, store, m, acc):
        for part in range(2):
            w = jnp.exp2(store[256 * part : 256 * part + 256] - m).astype(BF16)
            acc = acc + dot(vt[i, part], w, 1, 0)
        return acc

    def finish(first, acc):
        out = acc[:64] / acc[64:65]
        out = jnp.concatenate([out, jnp.zeros((64, 256), F32)], axis=0).T
        for a in range(4):
            top, low = out[64 * a : 64 * a + 32], out[64 * a + 32 : 64 * a + 64]
            o_ref[first + a] = (top + pltpu.roll(low, 64, 1)).astype(BF16)

    def turn(i):
        for part, keys in enumerate(keys_of(i)):
            vt[i, part, :64] = keys.T[64:]

    def three(j, u):
        raw = (
            raw_scores(8 * j + u, 2 * j),
            raw_scores(8 * j + u, 2 * j + 1),
            raw_scores(8 * j + 4 + u, 2 * j + 1),
        )
        return raw, (-u * BLK, None, -u * BLK)

    def keep_three(raw, limits):
        return tuple(keep(raw[n], limits[n], s.at[n]) for n in range(3))

    def tiles(j, peaks):
        base = 8 * j

        def step(i, states):
            raw = [raw_scores(i + 1, 2 * j + slot) for slot in range(2)]
            done = []
            for slot in range(2):
                m, acc, peak = states[slot]
                new = jnp.maximum(m, peak)
                acc = weigh(i, s.at[slot], new, acc * jnp.exp2(m - new))
                done.append((new, acc, keep(raw[slot], None, s.at[slot])))
            return tuple(done)

        m = jnp.full((1, 256), sink, F32)
        carry = (m, zero), (m, zero), peaks
        for u in range(4):
            (m0, acc0), (m1, acc1), (p0, p1, p2) = carry
            if u < 3:
                raw, limits = three(j, u + 1)
            elif j:
                raw = [raw_scores(0, 2 * j), raw_scores(0, 2 * j + 1)]
            turn(base + u)
            turn(base + 4 + u)
            n0 = jnp.maximum(m0, p0)
            n1 = jnp.maximum(m1, jnp.maximum(p1, p2))
            acc0 = weigh(base + u, s.at[0], n0, acc0 * jnp.exp2(m0 - n0))
            acc1 = weigh(base + u, s.at[1], n1, acc1 * jnp.exp2(m1 - n1))
            acc1 = weigh(base + 4 + u, s.at[2], n1, acc1)
            if u < 3:
                peaks = keep_three(raw, limits)
            elif j:
                peaks = [keep(raw[n], None, s.at[n]) for n in range(2)]
            carry = (n0, acc0), (n1, acc1), peaks
        states = tuple((*carry[slot], carry[2][slot]) for slot in range(2))

        def eight(t, states):
            for n in range(8):
                states = step(8 * t + n, states)
            return states

        if j:
            states = lax.fori_loop(0, j, eight, states)
        if j < 3:
            peaks = keep_three(*three(j + 1, 0))
        for slot in range(2):
            finish(base + 4 * slot, states[slot][1])
        return peaks

    peaks = keep_three(*three(0, 0))
    for j in range(NBLK // 8):
        peaks = tiles(j, peaks)


def return_part(places, o_ref, out, held, own, send, recv):
    z, y, x, c = place()
    for b in range(NBLK):
        own[b] = o_ref[places[b]]
    held[z * 4 + y] = own[z * 4 + y]

    def copy(k, block, head, target):
        return pltpu.make_async_remote_copy(
            src_ref=own.at[block],
            dst_ref=held.at[head],
            send_sem=send.at[k],
            recv_sem=recv.at[k],
            device_id=target,
            device_id_type=MESH,
        )

    def sent(k):
        dz, dy = OFFSETS[k]
        zz, yy = (z + dz) % 8, (y + dy) % 4
        return copy(k, zz * 4 + yy, z * 4 + y, dev(zz, yy, x, c))

    for k in range(31):
        sent(k).start()
    for k, (dz, dy) in enumerate(OFFSETS):
        zz, yy = (z + 8 - dz) % 8, (y + 4 - dy) % 4
        copy(k, 0, zz * 4 + yy, dev(zz, yy, x, c)).wait_recv()
    lane = lax.broadcasted_iota(I32, (32, 128), 1)
    for k in range(16):
        p, q = held[2 * k].astype(F32), held[2 * k + 1].astype(F32)
        cols = pl.ds(128 * k, 128)
        out[:32, cols] = jnp.where(lane < 64, p, pltpu.roll(q, 64, 1)).astype(BF16)
        out[32:, cols] = jnp.where(lane < 64, pltpu.roll(p, 64, 1), q).astype(BF16)
    for k in range(31):
        sent(k).wait_send()


def kernel(
    places_hbm, sinks_hbm, row_hbm, col_hbm, tok_hbm, wqt_hbm, kvw_hbm, out,
    places, sinks, inv_row, inv_col, ssem,
    q, kv, order, tok, wts, kvw, kvp, stage, mid, angles,
    lsem, send, recv, zsend, zrecv, psend, precv, ysend, yrecv, qsend, qrecv, known,
    attended, vt, qt, gap, s, held, own, osend, orecv,
):
    small = [
        pltpu.make_async_copy(places_hbm, places, ssem.at[0]),
        pltpu.make_async_copy(sinks_hbm, sinks, ssem.at[1]),
        pltpu.make_async_copy(row_hbm, inv_row, ssem.at[2]),
        pltpu.make_async_copy(col_hbm, inv_col, ssem.at[3]),
    ]
    prepare_part(
        lambda: attend_tables(vt, gap), lambda: attend_queries(q, order, qt),
        small, places, inv_row, inv_col, tok_hbm, wqt_hbm, kvw_hbm, q, kv, order,
        tok, wts, kvw, kvp, stage, mid, angles,
        lsem, send, recv, zsend, zrecv, psend, precv, ysend, yrecv, qsend, qrecv, known,
    )
    attend_part(sinks, kv, attended, order, vt, qt, gap, s)
    return_part(places, attended, out, held, own, osend, orecv)


def per_device(tokens, query_weight, key_value_weight, block_places, sinks):
    dma = pltpu.SemaphoreType.DMA
    return pl.pallas_call(
        kernel,
        in_specs=[HBM] * 7,
        out_specs=VMEM,
        out_shape=jax.ShapeDtypeStruct((64, 2048), BF16),
        scratch_shapes=[
            pltpu.SMEM((NBLK,), I32),
            pltpu.SMEM((32,), F32),
            pltpu.VMEM((1, 128), F32),
            pltpu.VMEM((32, 128), F32),
            dma((4,)),
            pltpu.VMEM((8, 64, 256), BF16),
            pltpu.VMEM((2, 4, 4, 8, 64, 128), BF16),
            pltpu.SMEM((NBLK,), I32),
            pltpu.VMEM((4, 2, 32, WIDTH), BF16),
            pltpu.VMEM((4, 2, 2, 32, WIDTH), BF16),
            pltpu.VMEM((WIDTH, 1024), BF16),
            pltpu.VMEM((8, 64, 128), BF16),
            pltpu.VMEM((4, 2, 64, 256), BF16),
            pltpu.VMEM((8, 64, 256), BF16),
            pltpu.VMEM((2, 32, 256), F32),
            dma((6,)),
            dma((42,)),
            dma((42,)),
            dma((7,)),
            dma((7,)),
            dma((20,)),
            dma((20,)),
            dma((8,)),
            dma((8,)),
            dma((8,)),
            dma((8,)),
            pltpu.SemaphoreType.REGULAR((4,)),
            pltpu.VMEM((NBLK, 32, 128), BF16),
            pltpu.VMEM((NBLK, 2, 80, 256), BF16),
            pltpu.VMEM((8, 128, 256), BF16),
            pltpu.VMEM((BLK, 256), I32),
            pltpu.VMEM((3, BLK, 256), F32),
            pltpu.VMEM((NBLK, 32, 128), BF16),
            pltpu.VMEM((NBLK, 32, 128), BF16),
            dma((31,)),
            dma((31,)),
        ],
        compiler_params=pltpu.CompilerParams(collective_id=1, has_side_effects=True),
        name="layer",
    )(
        block_places,
        sinks,
        jnp.asarray(np.tile(INVERSE, 4)[None, :]),
        jnp.asarray(np.tile(INVERSE[:, None], (1, 128))),
        tokens.reshape(2, 32, WIDTH),
        query_weight.T.reshape(2, 32, WIDTH),
        key_value_weight,
    )


def solution(mesh):
    in_specs = (P(("grp", "sp"), None), P(None, "sp"), P(), P(), P())
    return jax.shard_map(
        per_device,
        mesh=mesh,
        in_specs=in_specs,
        out_specs=P(("grp", "sp"), None),
        check_vma=False,
    )
```
